32 devices in a mesh: dp: 4 (over y, z), ep: 8 (over x, core).
Axes of the slice: x: 4, y: 2, z: 2, core: 2. Of those that a mesh axis runs over, the one named last changes fastest.
The devices are a block of a 4x4x8 slice.
Arguments:
- x_rows: bfloat16 [1024, 1536], P(('dp', 'ep')), parts along dimension 0
- expert_idx: int32 [1024, 8], P(('dp', 'ep')), parts along dimension 0
- gate_w: float32 [1024, 8], P(('dp', 'ep')), parts along dimension 0
- slot_pos: int32 [1024, 8], P(('dp', 'ep')), parts along dimension 0
- w_gate: bfloat16 [40, 1536, 512], P('ep')
- w_up: bfloat16 [40, 1536, 512], P('ep')
- w_down: bfloat16 [40, 512, 1536], P('ep')
- grad_out: bfloat16 [1024, 1536], P(('dp', 'ep')), parts along dimension 0
Outputs:
- output 1: bfloat16 [1024, 1536], P(('dp', 'ep')), parts along dimension 0
- output 2: bfloat16 [1024, 1536], P(('dp', 'ep')), parts along dimension 0
- output 3: bfloat16 [160, 1536, 512], P(('dp', 'ep')), parts along dimension 0
- output 4: bfloat16 [160, 1536, 512], P(('dp', 'ep')), parts along dimension 0
- output 5: bfloat16 [160, 512, 1536], P(('dp', 'ep')), parts along dimension 0
- output 6: float32 [1024, 8], P(('dp', 'ep')), parts along dimension 0
There are 4 independent parts. The reference program is written for one: setup_inputs(seed, part) draws one part's arguments, and reference() takes and returns one part's arrays. A program takes and returns all parts, laid end to end along the dimension named above; an argument that names none is the same for every part.
All inputs are finite; a program needn't handle non-finite values.
Results may differ from the reference program's by a relative error of at most 0.0103429.
Values are sent between devices in bfloat16 or wider.
A program may use at most 768 MiB of HBM per device.

```python
import jax
import jax.numpy as jnp
from jax import lax

TOK = 32
D = 1536
FF = 512
EXPERTS = 40
TOP = 8
GROUP = 8

CAP = ((2 * TOK * TOP + EXPERTS - 1) // EXPERTS + 7) // 8 * 8
HOT_ROWS = CAP + CAP // 4
TOKENS = GROUP * TOK
CHOICES = TOK * TOP
ROWS = EXPERTS * CAP


def rank_in_expert(expert_list):
    sort_order = jnp.argsort(expert_list, stable=True)
    ordered = expert_list[sort_order]
    first_pos = jnp.searchsorted(ordered, ordered)
    rank_sorted = (jnp.arange(CHOICES) - first_pos).astype(jnp.int32)
    return jnp.zeros((CHOICES,), jnp.int32).at[sort_order].set(rank_sorted)


def draw_routing(route_key):
    key_hot, key_rank, key_score = jax.random.split(route_key, 3)
    hot_expert = jax.random.randint(key_hot, (GROUP, 1, 1), 0, EXPERTS)
    tok_rank = jax.vmap(lambda sub_key: jax.random.permutation(sub_key, TOK))(jax.random.split(key_rank, GROUP))
    is_hot = (tok_rank < HOT_ROWS)[:, :, None]
    expert_ids = jnp.arange(EXPERTS, dtype=jnp.int32)
    base_score = jax.random.randint(key_score, (GROUP, TOK, EXPERTS), 0, 2 ** 20)
    hot_bonus = jnp.where(is_hot & (expert_ids == hot_expert), 2 ** 21, 0)
    score_int = (base_score + hot_bonus) * EXPERTS + expert_ids
    chosen = jnp.argsort(-score_int, axis=-1)[:, :, :TOP].astype(jnp.int32)
    rank_all = jax.vmap(rank_in_expert)(chosen.reshape(GROUP, CHOICES))
    slot_all = jnp.where(rank_all < CAP, rank_all, -1).astype(jnp.int32)
    return chosen.reshape(TOKENS, TOP), slot_all.reshape(TOKENS, TOP)


def setup_inputs(seed: int = 0, part: int = 0) -> dict:
    root_key = jax.random.key(seed)
    shared_key, data_key = jax.random.split(root_key)
    part_key = jax.random.fold_in(data_key, part)
    key_route, key_x, key_gate, key_grad = jax.random.split(part_key, 4)
    key_wg, key_wu, key_wd = jax.random.split(shared_key, 3)
    expert_idx, slot_pos = draw_routing(key_route)
    x_rows = jax.random.normal(key_x, (TOKENS, D), jnp.float32).astype(jnp.bfloat16)
    gate_w = jax.random.uniform(key_gate, (TOKENS, TOP), jnp.float32, 0.5, 1.5) * TOP ** -0.5
    w_gate = (jax.random.normal(key_wg, (EXPERTS, D, FF), jnp.float32) * D ** -0.5).astype(jnp.bfloat16)
    w_up = (jax.random.normal(key_wu, (EXPERTS, D, FF), jnp.float32) * D ** -0.5).astype(jnp.bfloat16)
    w_down = (jax.random.normal(key_wd, (EXPERTS, FF, D), jnp.float32) * FF ** -0.5).astype(jnp.bfloat16)
    grad_out = jax.random.normal(key_grad, (TOKENS, D), jnp.float32).astype(jnp.bfloat16)
    return {'x_rows': x_rows, 'expert_idx': expert_idx, 'gate_w': gate_w, 'slot_pos': slot_pos, 'w_gate': w_gate, 'w_up': w_up, 'w_down': w_down, 'grad_out': grad_out}


def take_rows(table, where_from):
    return jnp.take(table, where_from, axis=0, mode='fill', fill_value=0)


def to_experts(dev_rows):
    return dev_rows.reshape(GROUP, EXPERTS, CAP, D).transpose(1, 0, 2, 3).reshape(EXPERTS, GROUP * CAP, D)


def to_devices(exp_rows):
    return exp_rows.reshape(EXPERTS, GROUP, CAP, D).transpose(1, 0, 2, 3).reshape(GROUP, ROWS, D)


def expert_pass(operands):
    in_rows, dy_rows, gate_mat, up_mat, down_mat = operands
    pre_gate = jnp.dot(in_rows, gate_mat, preferred_element_type=jnp.float32)
    pre_up = jnp.dot(in_rows, up_mat, preferred_element_type=jnp.float32)
    gate_sig = jax.nn.sigmoid(pre_gate)
    gate_act = pre_gate * gate_sig
    hidden = (gate_act * pre_up).astype(jnp.bfloat16)
    out_exp = jnp.dot(hidden, down_mat, preferred_element_type=jnp.float32).astype(jnp.bfloat16)
    d_hidden = jnp.dot(dy_rows, down_mat.T, preferred_element_type=jnp.float32)
    d_gate = (d_hidden * pre_up * (gate_sig * (1.0 + pre_gate * (1.0 - gate_sig)))).astype(jnp.bfloat16)
    d_up = (d_hidden * gate_act).astype(jnp.bfloat16)
    g_down = jnp.dot(hidden.T, dy_rows, preferred_element_type=jnp.float32).astype(jnp.bfloat16)
    g_gate = jnp.dot(in_rows.T, d_gate, preferred_element_type=jnp.float32).astype(jnp.bfloat16)
    g_up = jnp.dot(in_rows.T, d_up, preferred_element_type=jnp.float32).astype(jnp.bfloat16)
    d_in = (jnp.dot(d_gate, gate_mat.T, preferred_element_type=jnp.float32) + jnp.dot(d_up, up_mat.T, preferred_element_type=jnp.float32)).astype(jnp.bfloat16)
    return out_exp, d_in, g_gate, g_up, g_down


def reference(x_rows, expert_idx, gate_w, slot_pos, w_gate, w_up, w_down, grad_out):
    flat_pos = jnp.where(slot_pos >= 0, expert_idx * CAP + slot_pos, ROWS).reshape(GROUP, CHOICES)
    choice_ids = jnp.arange(CHOICES, dtype=jnp.int32)
    src_choice = jax.vmap(lambda pos_row: jnp.full((ROWS,), CHOICES, jnp.int32).at[pos_row].set(choice_ids, mode='drop'))(flat_pos)
    src_tok = src_choice // TOP
    rows_of = jax.vmap(take_rows)
    sent_x = rows_of(x_rows.reshape(GROUP, TOK, D), src_tok)
    w_rows = rows_of(gate_w.reshape(GROUP, CHOICES), src_choice)
    g_rows = rows_of(grad_out.reshape(GROUP, TOK, D), src_tok)
    sent_dy = (w_rows[:, :, None] * g_rows.astype(jnp.float32)).astype(jnp.bfloat16)
    out_exp, d_in, grad_w_gate, grad_w_up, grad_w_down = lax.map(expert_pass, (to_experts(sent_x), to_experts(sent_dy), w_gate, w_up, w_down))
    y_choice = rows_of(to_devices(out_exp), flat_pos).reshape(TOKENS, TOP, D)
    d_choice = rows_of(to_devices(d_in), flat_pos).reshape(TOKENS, TOP, D)
    out_rows = jnp.sum(gate_w[:, :, None] * y_choice.astype(jnp.float32), axis=1).astype(jnp.bfloat16)
    grad_x = jnp.sum(d_choice.astype(jnp.float32), axis=1).astype(jnp.bfloat16)
    grad_gate = jnp.sum(grad_out[:, None, :].astype(jnp.float32) * y_choice.astype(jnp.float32), axis=-1)
    return out_rows, grad_x, grad_w_gate, grad_w_up, grad_w_down, grad_gate
```

```python
import functools

import jax
import jax.numpy as jnp
from jax import lax
from jax.experimental import pallas as pl
from jax.experimental.pallas import tpu as pltpu
from jax.sharding import PartitionSpec as P

BF16, F32 = jnp.bfloat16, jnp.float32
MESH_ID = pl.DeviceIdType.MESH
ANY = pl.ANY
LANES = 128


def capacity_of(tok_dev, top_k, n_experts):
    return ((2 * tok_dev * top_k + n_experts - 1) // n_experts + 7) // 8 * 8


def dot_nn(a, b):
    return lax.dot_general(a, b, (((1,), (0,)), ((), ())), preferred_element_type=F32)


def dot_nt(a, b):
    return lax.dot_general(a, b, (((1,), (1,)), ((), ())), preferred_element_type=F32)


def dot_tn(a, b):
    return lax.dot_general(a, b, (((0,), (0,)), ((), ())), preferred_element_type=F32)


def moe_kernel(dims, x_hbm, g_hbm, idx_ref, slot_ref, gate_ref, w1_hbm, w3_hbm, w2_hbm,
               out_ref, gx_ref, gg_ref, r_hbm, dy_hbm, h_hbm, da_hbm, db_hbm,
               w1, w3, w2, xg, meta, scr, scr2, r_all, dy_all, h_all, da_all, db_all, c1_all, c2_all,
               p_all, gs_all, y_all, dr_all, part, sibbuf, ringbuf, finbuf, ggsrc, ggbuf,
               w_sem, loc_sem, wb_sem, meta_ss, meta_rs, ag_ss, ag_rs, rt_ss, rt_rs, gg_ss, gg_rs):
    G, T, D, F, E, C, K = dims
    NQ = G // 2
    RW = G * C
    DH = D // 2
    per_tile = LANES // T
    me = lax.axis_index("ep")
    core = lax.rem(me, 2)
    chip = me // 2
    right_chip, left_chip, opp_chip = (lax.rem(chip + 1, NQ), lax.rem(chip + NQ - 1, NQ), lax.rem(chip + 2, NQ))
    dev = lambda q, c: q * 2 + c
    other = 1 - core
    sib = dev(chip, other)
    right, left, opp = dev(right_chip, core), dev(left_chip, core), dev(opp_chip, core)

    w_copies = []
    for e in range(E):
        for k, (src, dst) in enumerate(((w1_hbm, w1), (w3_hbm, w3), (w2_hbm, w2))):
            w_copies.append(pltpu.make_async_copy(src.at[e], dst.at[e], w_sem.at[k, e]))

    def rows(d):
        return pl.ds(pl.multiple_of(d * T, T), T)

    own_x = pltpu.make_async_copy(x_hbm, xg.at[0, rows(me)], loc_sem.at[0])
    own_g = pltpu.make_async_copy(g_hbm, xg.at[1, rows(me)], loc_sem.at[1])
    own_x.start()
    own_g.start()
    for cp in w_copies:
        cp.start()

    off = pl.multiple_of(lax.rem(me, per_tile) * T, T)
    scr[...] = jnp.zeros_like(scr)
    scr2[...] = jnp.zeros_like(scr2)
    code = jnp.where(slot_ref[...] >= 0, idx_ref[...] * C + slot_ref[...] + 1, 0)
    scr[pl.ds(off, T), 0:K] = code.astype(F32)
    scr2[pl.ds(off, T), 0:K] = gate_ref[...]
    meta[me, 0:K] = jnp.transpose(scr[...])[0:K]
    meta[me, K:2 * K] = jnp.transpose(scr2[...])[0:K]

    barrier = pltpu.get_barrier_semaphore()
    for d in range(1, G):
        pl.semaphore_signal(barrier, inc=1, device_id={"ep": lax.rem(me + d, G)}, device_id_type=MESH_ID)
    pl.semaphore_wait(barrier, G - 1)

    def remote(src, dst, ss, rs, target):
        return pltpu.make_async_remote_copy(src_ref=src, dst_ref=dst, send_sem=ss, recv_sem=rs,
                                            device_id={"ep": target}, device_id_type=MESH_ID)

    meta_sends = []
    for d in range(1, G):
        cp = remote(meta.at[me], meta.at[me], meta_ss.at[d - 1], meta_rs.at[d - 1], lax.rem(me + d, G))
        cp.start()
        meta_sends.append(cp)

    lo, hi, full = pl.ds(0, DH), pl.ds(DH, DH), pl.ds(0, D)

    def ag(t, k, src_dev, cols, target):
        ref = xg.at[t, rows(src_dev), cols]
        return remote(ref, ref, ag_ss.at[t, k], ag_rs.at[t, k], target)

    sib_right, sib_left, sib_opp = dev(right_chip, other), dev(left_chip, other), dev(opp_chip, other)
    send_desc = lambda t: [ag(t, 0, me, full, sib), ag(t, 1, me, lo, right), ag(t, 2, me, hi, right),
                           ag(t, 3, me, hi, left), ag(t, 4, me, lo, left),
                           ag(t, 5, left, lo, right), ag(t, 6, right, hi, left),
                           ag(t, 7, left, full, sib), ag(t, 8, right, full, sib),
                           ag(t, 9, opp, lo, sib), ag(t, 10, opp, hi, sib)]
    recv_desc = lambda t: [ag(t, 0, sib, full, sib), ag(t, 1, left, lo, left), ag(t, 2, left, hi, left),
                           ag(t, 3, right, hi, right), ag(t, 4, right, lo, right),
                           ag(t, 5, opp, lo, left), ag(t, 6, opp, hi, right),
                           ag(t, 7, sib_left, full, sib), ag(t, 8, sib_right, full, sib),
                           ag(t, 9, sib_opp, lo, sib), ag(t, 10, sib_opp, hi, sib)]
    sx, sg = send_desc(0), send_desc(1)
    rx, rg = recv_desc(0), recv_desc(1)

    own_x.wait()
    for k in (1, 3, 2, 4, 0):
        sx[k].start()
    own_g.wait()
    rx[1].wait_recv()
    sx[5].start()
    rx[3].wait_recv()
    sx[6].start()
    for k in (1, 3, 2, 4, 0):
        sg[k].start()
    rx[2].wait_recv()
    sx[7].start()
    rx[4].wait_recv()
    sx[8].start()
    rx[5].wait_recv()
    sx[9].start()
    rx[6].wait_recv()
    sx[10].start()
    for d in range(1, G):
        src = lax.rem(me + G - d, G)
        remote(meta.at[src], meta.at[src], meta_ss.at[d - 1], meta_rs.at[d - 1], src).wait_recv()
    for k in (0, 7, 8, 9, 10):
        rx[k].wait_recv()
    rg[1].wait_recv()
    sg[5].start()
    rg[3].wait_recv()
    sg[6].start()

    n_tiles = G // per_tile
    halves = []
    for i in range(n_tiles):
        tot = meta[i * per_tile]
        for s in range(i * per_tile + 1, (i + 1) * per_tile):
            tot = tot + meta[s]
        halves.append(tot)
    codes = jnp.concatenate([v[0:K] for v in halves], axis=1)
    gates = jnp.concatenate([v[K:2 * K] for v in halves], axis=1)
    NT = G * T
    lane_src = (lax.broadcasted_iota(jnp.int32, (K, NT), 1) // T * C).astype(F32)
    row_id = lax.broadcasted_iota(jnp.int32, (RW, NT), 0).astype(F32) + 1.0

    def routing(e):
        first = ((me * E + e) * C).astype(F32) + 1.0
        sel = (codes >= first) & (codes < first + float(C))
        pos = jnp.sum(jnp.where(sel, codes - first + lane_src + 1.0, 0.0), axis=0, keepdims=True)
        return sel, row_id == pos

    def erow(e):
        return pl.ds(pl.multiple_of(e * RW, RW), RW)

    def fwd(e, carry):
        sel, mask = routing(e)
        gate_row = jnp.sum(jnp.where(sel, gates, 0.0), axis=0, keepdims=True)
        p_e = jnp.where(mask, 1.0, 0.0).astype(BF16)
        p_all[erow(e), :] = p_e
        rest = gate_row
        for part_i in range(3):
            piece = rest.astype(BF16).astype(F32)
            gs_all[part_i, erow(e), :] = jnp.where(mask, piece, 0.0).astype(BF16)
            rest = rest - piece
        r_e = dot_nn(p_e, xg[0]).astype(BF16)
        r_all[e] = r_e
        for k in range(3):
            pltpu.make_async_copy((w1_hbm, w3_hbm, w2_hbm)[k].at[e], (w1, w3, w2)[k].at[e], w_sem.at[k, e]).wait()
        a = dot_nn(r_e, w1[e])
        b = dot_nn(r_e, w3[e])
        s = jax.nn.sigmoid(a)
        act = a * s
        h_e = (act * b).astype(BF16)
        h_all[e] = h_e
        c1_all[e] = b * (s * (1.0 + a * (1.0 - s)))
        c2_all[e] = act
        y_all[erow(e), :] = dot_nn(h_e, w2[e]).astype(BF16)

        @pl.when(e == 1)
        def _():
            rg[2].wait_recv()
            sg[7].start()
            rg[4].wait_recv()
            sg[8].start()

        @pl.when(e == 2)
        def _():
            rg[5].wait_recv()
            sg[9].start()
            rg[6].wait_recv()
            sg[10].start()

        return carry

    lax.fori_loop(0, E, fwd, 0)

    def back(t, n, src, dst, target):
        return remote(src, dst, rt_ss.at[t, n], rt_rs.at[t, n], target)

    chips = (opp_chip, right_chip, left_chip, chip)

    def ret_sib_send(t):
        return [back(t, i, part.at[t, rows(dev(q, other))], sibbuf.at[t, i], sib) for i, q in enumerate(chips)]

    def ret_ring_send(t):
        return [back(t, 4, part.at[t, rows(opp), lo], ringbuf.at[t, 0], right),
                back(t, 5, part.at[t, rows(opp), hi], ringbuf.at[t, 1], left),
                back(t, 6, part.at[t, rows(right), hi], finbuf.at[t, 0, :, hi], right),
                back(t, 7, part.at[t, rows(left), lo], finbuf.at[t, 1, :, lo], left),
                back(t, 8, part.at[t, rows(right), lo], finbuf.at[t, 0, :, lo], right),
                back(t, 9, part.at[t, rows(left), hi], finbuf.at[t, 1, :, hi], left)]

    def ret_1(t):
        sends, ring = ret_sib_send(t), ret_ring_send(t)
        for i, d in enumerate((opp, right, left)):
            sends[i].wait_recv()
            part[t, rows(d), :] += sibbuf[t, i]
            if i == 0:
                ring[0].start()
                ring[1].start()
            if i == 1:
                ring[2].start()
            if i == 2:
                ring[3].start()
        sends[3].wait_recv()
        part[t, rows(me), :] += sibbuf[t, 3]

    def ret_2(t):
        ring = ret_ring_send(t)
        ring[0].wait_recv()
        part[t, rows(right), lo] += ringbuf[t, 0]
        ring[4].start()
        ring[1].wait_recv()
        part[t, rows(left), hi] += ringbuf[t, 1]
        ring[5].start()

    def ret_3(t, res_ref):
        ring = ret_ring_send(t)
        for n in (2, 3, 4, 5):
            ring[n].wait_recv()
        res_ref[...] = (part[t, rows(me), :] + finbuf[t, 0] + finbuf[t, 1]).astype(BF16)
        for cp in ret_sib_send(t) + ring:
            cp.wait_send()

    acc = dot_tn(gs_all[0], y_all[...])
    for i in (1, 2):
        acc = acc + dot_tn(gs_all[i], y_all[...])
    part[0] = acc
    for cp in ret_sib_send(0):
        cp.start()

    for k in (0, 7, 8, 9, 10):
        rg[k].wait_recv()

    def bwd(e, gg):
        sel, mask = routing(e)
        gate_row = jnp.sum(jnp.where(sel, gates, 0.0), axis=0, keepdims=True)
        gate_col = jnp.sum(jnp.where(mask, gate_row, 0.0), axis=1, keepdims=True)
        g_e = dot_nn(p_all[erow(e), :], xg[1])
        gg_col = jnp.sum(g_e * y_all[erow(e), :].astype(F32), axis=1, keepdims=True)
        gg_row = jnp.sum(jnp.where(mask, gg_col, 0.0), axis=0, keepdims=True)
        gg = gg + jnp.where(sel, gg_row, 0.0)
        dy_e = (gate_col * g_e).astype(BF16)
        dy_all[e] = dy_e
        dh = dot_nt(dy_e, w2[e])
        da_e = (dh * c1_all[e]).astype(BF16)
        db_e = (dh * c2_all[e]).astype(BF16)
        da_all[e] = da_e
        db_all[e] = db_e
        dr_all[erow(e), :] = (dot_nt(da_e, w1[e]) + dot_nt(db_e, w3[e])).astype(BF16)

        @pl.when(e == 1)
        def _():
            ret_1(0)

        @pl.when(e == 3)
        def _():
            ret_2(0)

        return gg

    gg = lax.fori_loop(0, E, bwd, jnp.zeros((K, NT), F32))
    for i in range(n_tiles):
        ggsrc[i] = gg[:, i * LANES:(i + 1) * LANES]
    part[1] = dot_tn(p_all[...], dr_all[...])
    for cp in ret_sib_send(1):
        cp.start()
    gg_sends = []
    for d in range(1, G):
        tgt = lax.rem(me + d, G)
        cp = remote(ggsrc.at[tgt // per_tile], ggbuf.at[d - 1], gg_ss.at[d - 1], gg_rs.at[d - 1], tgt)
        cp.start()
        gg_sends.append(cp)
    wb = [pltpu.make_async_copy(src, dst, wb_sem.at[i]) for i, (src, dst) in enumerate(
        ((r_all, r_hbm), (dy_all, dy_hbm), (h_all, h_hbm), (da_all, da_hbm), (db_all, db_hbm)))]
    for cp in wb:
        cp.start()
    ret_3(0, out_ref)
    ret_1(1)
    tot = ggsrc[me // per_tile]
    for d in range(1, G):
        gg_sends[d - 1].wait_recv()
        tot = tot + ggbuf[d - 1]
    scr[0:K, :] = tot
    scr2[...] = jnp.transpose(scr[...])
    gg_ref[...] = scr2[pl.ds(off, T), 0:K]
    ret_2(1)
    for cp in meta_sends + sx + sg + gg_sends:
        cp.wait_send()
    for cp in wb:
        cp.wait()
    ret_3(1, gx_ref)


def wgrad_kernel(r_ref, dy_ref, h_ref, da_ref, db_ref, o_in, gx_in, gg_in,
                 g1_ref, g3_ref, g2_ref, o_ref, gx_ref, gg_ref):
    r = r_ref[...]
    g1_ref[...] = dot_tn(r, da_ref[...]).astype(BF16)
    g3_ref[...] = dot_tn(r, db_ref[...]).astype(BF16)
    g2_ref[...] = dot_tn(h_ref[...], dy_ref[...]).astype(BF16)

    @pl.when(pl.program_id(0) == 0)
    def _():
        o_ref[...] = o_in[...]
        gx_ref[...] = gx_in[...]
        gg_ref[...] = gg_in[...]


def solution(mesh):
    group_size = mesh.shape['ep']
    row_spec = P(('dp', 'ep'))
    expert_spec = P('ep')

    def per_device(x_rows, expert_idx, gate_w, slot_pos, w_gate, w_up, w_down, grad_out):
        T, D = x_rows.shape
        K = expert_idx.shape[1]
        E, _, F = w_gate.shape
        G = group_size
        C = capacity_of(T, K, E * G)
        RW, NT = G * C, G * T
        NQ = G // 2
        dims = (G, T, D, F, E, C, K)
        sds = jax.ShapeDtypeStruct
        vm = pltpu.VMEM
        dma = pltpu.SemaphoreType.DMA
        vspec = pl.BlockSpec(memory_space=pltpu.VMEM)
        aspec = pl.BlockSpec(memory_space=ANY)
        out, gx, gg, r, dy, h, da, db = pl.pallas_call(
            functools.partial(moe_kernel, dims),
            out_shape=(sds((T, D), BF16), sds((T, D), BF16), sds((T, K), F32),
                       sds((E, RW, D), BF16), sds((E, RW, D), BF16),
                       sds((E, RW, F), BF16), sds((E, RW, F), BF16), sds((E, RW, F), BF16)),
            in_specs=[aspec, aspec, vspec, vspec, vspec, aspec, aspec, aspec],
            out_specs=(vspec, vspec, vspec, aspec, aspec, aspec, aspec, aspec),
            scratch_shapes=[
                vm((E, D, F), BF16), vm((E, D, F), BF16), vm((E, F, D), BF16),
                vm((2, NT, D), BF16), vm((G, 2 * K, LANES), F32),
                vm((LANES, LANES), F32), vm((LANES, LANES), F32),
                vm((E, RW, D), BF16), vm((E, RW, D), BF16),
                vm((E, RW, F), BF16), vm((E, RW, F), BF16), vm((E, RW, F), BF16),
                vm((E, RW, F), F32), vm((E, RW, F), F32),
                vm((E * RW, NT), BF16), vm((3, E * RW, NT), BF16),
                vm((E * RW, D), BF16), vm((E * RW, D), BF16),
                vm((2, NT, D), F32), vm((2, NQ, T, D), F32),
                vm((2, 2, T, D // 2), F32), vm((2, 2, T, D), F32),
                vm((NT // LANES, K, LANES), F32), vm((G - 1, K, LANES), F32),
                dma((3, E)), dma((2,)), dma((5,)), dma((G - 1,)), dma((G - 1,)),
                dma((2, 11)), dma((2, 11)), dma((2, 10)), dma((2, 10)), dma((G - 1,)), dma((G - 1,)),
            ],
            compiler_params=pltpu.CompilerParams(
                collective_id=0, has_side_effects=True, vmem_limit_bytes=60 * 2 ** 20),
            name="moe_exchange",
        )(x_rows, grad_out, expert_idx, slot_pos, gate_w, w_gate, w_up, w_down)

        blk = lambda *s: pl.BlockSpec((pl.Squeezed(),) + s, lambda e: (e,) + (0,) * len(s))
        whole = lambda *s: pl.BlockSpec(s, lambda e: (0,) * len(s))
        g1, g3, g2, out, gx, gg = pl.pallas_call(
            wgrad_kernel,
            grid=(E,),
            out_shape=(sds((E, D, F), BF16), sds((E, D, F), BF16), sds((E, F, D), BF16),
                       sds((T, D), BF16), sds((T, D), BF16), sds((T, K), F32)),
            in_specs=[blk(RW, D), blk(RW, D), blk(RW, F), blk(RW, F), blk(RW, F),
                      whole(T, D), whole(T, D), whole(T, K)],
            out_specs=(blk(D, F), blk(D, F), blk(F, D), whole(T, D), whole(T, D), whole(T, K)),
            compiler_params=pltpu.CompilerParams(vmem_limit_bytes=40 * 2 ** 20),
            name="weight_grads",
        )(r, dy, h, da, db, out, gx, gg)
        return out, gx, g1, g3, g2, gg

    return jax.shard_map(per_device, mesh=mesh,
                         in_specs=(row_spec, row_spec, row_spec, row_spec, expert_spec, expert_spec, expert_spec, row_spec),
                         out_specs=(row_spec, row_spec, row_spec, row_spec, row_spec, row_spec),
                         check_vma=False)
```

```python
import functools

import jax
import jax.numpy as jnp
from jax import lax
from jax.experimental import pallas as pl
from jax.experimental.pallas import tpu as pltpu
from jax.sharding import PartitionSpec as P

BF16, F32 = jnp.bfloat16, jnp.float32
MESH_ID = pl.DeviceIdType.MESH
ANY = pl.ANY
LANES = 128


def capacity_of(tok_dev, top_k, n_experts):
    return ((2 * tok_dev * top_k + n_experts - 1) // n_experts + 7) // 8 * 8


def dot_nn(a, b):
    return lax.dot_general(a, b, (((1,), (0,)), ((), ())), preferred_element_type=F32)


def dot_nt(a, b):
    return lax.dot_general(a, b, (((1,), (1,)), ((), ())), preferred_element_type=F32)


def dot_tn(a, b):
    return lax.dot_general(a, b, (((0,), (0,)), ((), ())), preferred_element_type=F32)


def moe_kernel(dims, x_hbm, g_hbm, idx_ref, slot_ref, gate_ref, w1_hbm, w3_hbm, w2_hbm,
               out_ref, gx_ref, gg_ref, r_hbm, dy_hbm, h_hbm, da_hbm, db_hbm,
               w1, w3, w2, xg, meta, scr, r_all, dy_all, h_all, da_all, db_all, c1_all, c2_all,
               p_all, gs_all, y_all, dr_all, part, sibbuf, ringbuf, finbuf, ggsrc, ggbuf,
               w_sem, loc_sem, wb_sem, meta_ss, meta_rs, ag_ss, ag_rs, rt_ss, rt_rs, gg_ss, gg_rs):
    G, T, D, F, E, C, K = dims
    NQ = G // 2
    RW = G * C
    DH = D // 2
    per_tile = LANES // T
    me = lax.axis_index("ep")
    core = lax.rem(me, 2)
    chip = me // 2
    right_chip, left_chip, opp_chip = (lax.rem(chip + 1, NQ), lax.rem(chip + NQ - 1, NQ), lax.rem(chip + 2, NQ))
    dev = lambda q, c: q * 2 + c
    other = 1 - core
    sib = dev(chip, other)
    right, left, opp = dev(right_chip, core), dev(left_chip, core), dev(opp_chip, core)

    w_copies = []
    for e in range(E):
        for k, (src, dst) in enumerate(((w1_hbm, w1), (w3_hbm, w3), (w2_hbm, w2))):
            w_copies.append(pltpu.make_async_copy(src.at[e], dst.at[e], w_sem.at[k, e]))

    def rows(d):
        return pl.ds(pl.multiple_of(d * T, T), T)

    own_x = pltpu.make_async_copy(x_hbm, xg.at[0, rows(me)], loc_sem.at[0])
    own_g = pltpu.make_async_copy(g_hbm, xg.at[1, rows(me)], loc_sem.at[1])
    own_x.start()
    own_g.start()
    for cp in w_copies:
        cp.start()

    off = lax.rem(me, per_tile) * T
    scr[...] = jnp.zeros_like(scr)
    scr[0:K, 0:T] = jnp.where(slot_ref[...] >= 0, idx_ref[...] * C + slot_ref[...] + 1, 0).astype(F32)
    scr[K:2 * K, 0:T] = gate_ref[...]
    meta[me] = pltpu.roll(scr[...], off, 1)

    barrier = pltpu.get_barrier_semaphore()
    for d in range(1, G):
        pl.semaphore_signal(barrier, inc=1, device_id={"ep": lax.rem(me + d, G)}, device_id_type=MESH_ID)
    pl.semaphore_wait(barrier, G - 1)

    def remote(src, dst, ss, rs, target):
        return pltpu.make_async_remote_copy(src_ref=src, dst_ref=dst, send_sem=ss, recv_sem=rs,
                                            device_id={"ep": target}, device_id_type=MESH_ID)

    meta_sends = []
    for d in range(1, G):
        cp = remote(meta.at[me], meta.at[me], meta_ss.at[d - 1], meta_rs.at[d - 1], lax.rem(me + d, G))
        cp.start()
        meta_sends.append(cp)

    lo, hi, full = pl.ds(0, DH), pl.ds(DH, DH), pl.ds(0, D)

    def ag(t, k, src_dev, cols, target):
        ref = xg.at[t, rows(src_dev), cols]
        return remote(ref, ref, ag_ss.at[t, k], ag_rs.at[t, k], target)

    sib_right, sib_left, sib_opp = dev(right_chip, other), dev(left_chip, other), dev(opp_chip, other)
    send_desc = lambda t: [ag(t, 0, me, full, sib), ag(t, 1, me, lo, right), ag(t, 2, me, hi, right),
                           ag(t, 3, me, hi, left), ag(t, 4, me, lo, left),
                           ag(t, 5, left, lo, right), ag(t, 6, right, hi, left),
                           ag(t, 7, left, full, sib), ag(t, 8, right, full, sib),
                           ag(t, 9, opp, lo, sib), ag(t, 10, opp, hi, sib)]
    recv_desc = lambda t: [ag(t, 0, sib, full, sib), ag(t, 1, left, lo, left), ag(t, 2, left, hi, left),
                           ag(t, 3, right, hi, right), ag(t, 4, right, lo, right),
                           ag(t, 5, opp, lo, left), ag(t, 6, opp, hi, right),
                           ag(t, 7, sib_left, full, sib), ag(t, 8, sib_right, full, sib),
                           ag(t, 9, sib_opp, lo, sib), ag(t, 10, sib_opp, hi, sib)]
    sx, sg = send_desc(0), send_desc(1)
    rx, rg = recv_desc(0), recv_desc(1)

    own_x.wait()
    for k in (1, 3, 2, 4, 0):
        sx[k].start()
    own_g.wait()
    rx[1].wait_recv()
    sx[5].start()
    rx[3].wait_recv()
    sx[6].start()
    for k in (1, 3, 2, 4, 0):
        sg[k].start()
    rx[2].wait_recv()
    sx[7].start()
    rx[4].wait_recv()
    sx[8].start()
    rx[5].wait_recv()
    sx[9].start()
    rx[6].wait_recv()
    sx[10].start()
    for d in range(1, G):
        src = lax.rem(me + G - d, G)
        remote(meta.at[src], meta.at[src], meta_ss.at[d - 1], meta_rs.at[d - 1], src).wait_recv()
    for k in (0, 7, 8, 9, 10):
        rx[k].wait_recv()
    rg[1].wait_recv()
    sg[5].start()
    rg[3].wait_recv()
    sg[6].start()

    n_tiles = G // per_tile
    halves = []
    for i in range(n_tiles):
        tot = meta[i * per_tile]
        for s in range(i * per_tile + 1, (i + 1) * per_tile):
            tot = tot + meta[s]
        halves.append(tot)
    codes = jnp.concatenate([v[0:K] for v in halves], axis=1)
    gates = jnp.concatenate([v[K:2 * K] for v in halves], axis=1)
    NT = G * T
    lane_src = (lax.broadcasted_iota(jnp.int32, (K, NT), 1) // T * C).astype(F32)
    row_id = lax.broadcasted_iota(jnp.int32, (RW, NT), 0).astype(F32) + 1.0

    def routing(e):
        first = ((me * E + e) * C).astype(F32) + 1.0
        sel = (codes >= first) & (codes < first + float(C))
        pos = jnp.sum(jnp.where(sel, codes - first + lane_src + 1.0, 0.0), axis=0, keepdims=True)
        return sel, row_id == pos

    def erow(e):
        return pl.ds(pl.multiple_of(e * RW, RW), RW)

    def fwd(e, carry):
        sel, mask = routing(e)
        gate_row = jnp.sum(jnp.where(sel, gates, 0.0), axis=0, keepdims=True)
        p_e = jnp.where(mask, 1.0, 0.0).astype(BF16)
        p_all[erow(e), :] = p_e
        rest = gate_row
        for part_i in range(3):
            piece = rest.astype(BF16).astype(F32)
            gs_all[part_i, erow(e), :] = jnp.where(mask, piece, 0.0).astype(BF16)
            rest = rest - piece
        r_e = dot_nn(p_e, xg[0]).astype(BF16)
        r_all[e] = r_e
        for k in range(3):
            pltpu.make_async_copy((w1_hbm, w3_hbm, w2_hbm)[k].at[e], (w1, w3, w2)[k].at[e], w_sem.at[k, e]).wait()
        a = dot_nn(r_e, w1[e])
        b = dot_nn(r_e, w3[e])
        s = jax.nn.sigmoid(a)
        act = a * s
        h_e = (act * b).astype(BF16)
        h_all[e] = h_e
        c1_all[e] = b * (s * (1.0 + a * (1.0 - s)))
        c2_all[e] = act
        y_all[erow(e), :] = dot_nn(h_e, w2[e]).astype(BF16)

        @pl.when(e == 1)
        def _():
            rg[2].wait_recv()
            sg[7].start()
            rg[4].wait_recv()
            sg[8].start()

        @pl.when(e == 2)
        def _():
            rg[5].wait_recv()
            sg[9].start()
            rg[6].wait_recv()
            sg[10].start()

        return carry

    lax.fori_loop(0, E, fwd, 0)

    def back(t, n, src, dst, target):
        return remote(src, dst, rt_ss.at[t, n], rt_rs.at[t, n], target)

    chips = (opp_chip, right_chip, left_chip, chip)

    def ret_sib_send(t):
        return [back(t, i, part.at[t, rows(dev(q, other))], sibbuf.at[t, i], sib) for i, q in enumerate(chips)]

    def ret_ring_send(t):
        return [back(t, 4, part.at[t, rows(opp), lo], ringbuf.at[t, 0], right),
                back(t, 5, part.at[t, rows(opp), hi], ringbuf.at[t, 1], left),
                back(t, 6, part.at[t, rows(right), hi], finbuf.at[t, 0, :, hi], right),
                back(t, 7, part.at[t, rows(left), lo], finbuf.at[t, 1, :, lo], left),
                back(t, 8, part.at[t, rows(right), lo], finbuf.at[t, 0, :, lo], right),
                back(t, 9, part.at[t, rows(left), hi], finbuf.at[t, 1, :, hi], left)]

    def ret_1(t):
        sends, ring = ret_sib_send(t), ret_ring_send(t)
        for i, d in enumerate((opp, right, left)):
            sends[i].wait_recv()
            part[t, rows(d), :] += sibbuf[t, i]
            if i == 0:
                ring[0].start()
                ring[1].start()
            if i == 1:
                ring[2].start()
            if i == 2:
                ring[3].start()
        sends[3].wait_recv()
        part[t, rows(me), :] += sibbuf[t, 3]

    def ret_2(t):
        ring = ret_ring_send(t)
        ring[0].wait_recv()
        part[t, rows(right), lo] += ringbuf[t, 0]
        ring[4].start()
        ring[1].wait_recv()
        part[t, rows(left), hi] += ringbuf[t, 1]
        ring[5].start()

    def ret_3(t, res_ref):
        ring = ret_ring_send(t)
        for n in (2, 3, 4, 5):
            ring[n].wait_recv()
        res_ref[...] = (part[t, rows(me), :] + finbuf[t, 0] + finbuf[t, 1]).astype(BF16)
        for cp in ret_sib_send(t) + ring:
            cp.wait_send()

    acc = dot_tn(gs_all[0], y_all[...])
    for i in (1, 2):
        acc = acc + dot_tn(gs_all[i], y_all[...])
    part[0] = acc
    for cp in ret_sib_send(0):
        cp.start()

    for k in (0, 7, 8, 9, 10):
        rg[k].wait_recv()

    def bwd(e, gg):
        sel, mask = routing(e)
        gate_row = jnp.sum(jnp.where(sel, gates, 0.0), axis=0, keepdims=True)
        gate_col = jnp.sum(jnp.where(mask, gate_row, 0.0), axis=1, keepdims=True)
        g_e = dot_nn(p_all[erow(e), :], xg[1])
        gg_col = jnp.sum(g_e * y_all[erow(e), :].astype(F32), axis=1, keepdims=True)
        gg_row = jnp.sum(jnp.where(mask, gg_col, 0.0), axis=0, keepdims=True)
        gg = gg + jnp.where(sel, gg_row, 0.0)
        dy_e = (gate_col * g_e).astype(BF16)
        dy_all[e] = dy_e
        dh = dot_nt(dy_e, w2[e])
        da_e = (dh * c1_all[e]).astype(BF16)
        db_e = (dh * c2_all[e]).astype(BF16)
        da_all[e] = da_e
        db_all[e] = db_e
        dr_all[erow(e), :] = (dot_nt(da_e, w1[e]) + dot_nt(db_e, w3[e])).astype(BF16)

        @pl.when(e == 1)
        def _():
            ret_1(0)

        @pl.when(e == 3)
        def _():
            ret_2(0)

        return gg

    gg = lax.fori_loop(0, E, bwd, jnp.zeros((K, NT), F32))
    for i in range(n_tiles):
        ggsrc[i] = gg[:, i * LANES:(i + 1) * LANES]
    part[1] = dot_tn(p_all[...], dr_all[...])
    for cp in ret_sib_send(1):
        cp.start()
    gg_sends = []
    for d in range(1, G):
        tgt = lax.rem(me + d, G)
        cp = remote(ggsrc.at[tgt // per_tile], ggbuf.at[d - 1], gg_ss.at[d - 1], gg_rs.at[d - 1], tgt)
        cp.start()
        gg_sends.append(cp)
    wb = [pltpu.make_async_copy(src, dst, wb_sem.at[i]) for i, (src, dst) in enumerate(
        ((r_all, r_hbm), (dy_all, dy_hbm), (h_all, h_hbm), (da_all, da_hbm), (db_all, db_hbm)))]
    for cp in wb:
        cp.start()
    ret_3(0, out_ref)
    ret_1(1)
    tot = ggsrc[me // per_tile]
    for d in range(1, G):
        gg_sends[d - 1].wait_recv()
        tot = tot + ggbuf[d - 1]
    gg_ref[...] = pltpu.roll(tot, lax.rem(LANES - off, LANES), 1)[:, 0:T]
    ret_2(1)
    for cp in meta_sends + sx + sg + gg_sends:
        cp.wait_send()
    for cp in wb:
        cp.wait()
    ret_3(1, gx_ref)


def wgrad_kernel(r_ref, dy_ref, h_ref, da_ref, db_ref, o_in, gx_in, gg_in,
                 g1_ref, g3_ref, g2_ref, o_ref, gx_ref, gg_ref):
    r = r_ref[...]
    g1_ref[...] = dot_tn(r, da_ref[...]).astype(BF16)
    g3_ref[...] = dot_tn(r, db_ref[...]).astype(BF16)
    g2_ref[...] = dot_tn(h_ref[...], dy_ref[...]).astype(BF16)

    @pl.when(pl.program_id(0) == 0)
    def _():
        o_ref[...] = o_in[...]
        gx_ref[...] = gx_in[...]
        gg_ref[...] = gg_in[...]


def solution(mesh):
    group_size = mesh.shape['ep']
    row_spec = P(('dp', 'ep'))
    expert_spec = P('ep')

    def per_device(x_rows, expert_idx, gate_w, slot_pos, w_gate, w_up, w_down, grad_out):
        T, D = x_rows.shape
        K = expert_idx.shape[1]
        E, _, F = w_gate.shape
        G = group_size
        C = capacity_of(T, K, E * G)
        RW, NT = G * C, G * T
        NQ = G // 2
        dims = (G, T, D, F, E, C, K)
        sds = jax.ShapeDtypeStruct
        vm = pltpu.VMEM
        dma = pltpu.SemaphoreType.DMA
        vspec = pl.BlockSpec(memory_space=pltpu.VMEM)
        aspec = pl.BlockSpec(memory_space=ANY)
        out, gx, gg, r, dy, h, da, db = pl.pallas_call(
            functools.partial(moe_kernel, dims),
            out_shape=(sds((T, D), BF16), sds((T, D), BF16), sds((K, T), F32),
                       sds((E, RW, D), BF16), sds((E, RW, D), BF16),
                       sds((E, RW, F), BF16), sds((E, RW, F), BF16), sds((E, RW, F), BF16)),
            in_specs=[aspec, aspec, vspec, vspec, vspec, aspec, aspec, aspec],
            out_specs=(vspec, vspec, vspec, aspec, aspec, aspec, aspec, aspec),
            scratch_shapes=[
                vm((E, D, F), BF16), vm((E, D, F), BF16), vm((E, F, D), BF16),
                vm((2, NT, D), BF16), vm((G, 2 * K, LANES), F32),
                vm((2 * K, LANES), F32),
                vm((E, RW, D), BF16), vm((E, RW, D), BF16),
                vm((E, RW, F), BF16), vm((E, RW, F), BF16), vm((E, RW, F), BF16),
                vm((E, RW, F), F32), vm((E, RW, F), F32),
                vm((E * RW, NT), BF16), vm((3, E * RW, NT), BF16),
                vm((E * RW, D), BF16), vm((E * RW, D), BF16),
                vm((2, NT, D), F32), vm((2, NQ, T, D), F32),
                vm((2, 2, T, D // 2), F32), vm((2, 2, T, D), F32),
                vm((NT // LANES, K, LANES), F32), vm((G - 1, K, LANES), F32),
                dma((3, E)), dma((2,)), dma((5,)), dma((G - 1,)), dma((G - 1,)),
                dma((2, 11)), dma((2, 11)), dma((2, 10)), dma((2, 10)), dma((G - 1,)), dma((G - 1,)),
            ],
            compiler_params=pltpu.CompilerParams(
                collective_id=0, has_side_effects=True, vmem_limit_bytes=60 * 2 ** 20),
            name="moe_exchange",
        )(x_rows, grad_out, expert_idx.T, slot_pos.T, gate_w.T, w_gate, w_up, w_down)

        blk = lambda *s: pl.BlockSpec((pl.Squeezed(),) + s, lambda e: (e,) + (0,) * len(s))
        whole = lambda *s: pl.BlockSpec(s, lambda e: (0,) * len(s))
        g1, g3, g2, out, gx, gg = pl.pallas_call(
            wgrad_kernel,
            grid=(E,),
            out_shape=(sds((E, D, F), BF16), sds((E, D, F), BF16), sds((E, F, D), BF16),
                       sds((T, D), BF16), sds((T, D), BF16), sds((K, T), F32)),
            in_specs=[blk(RW, D), blk(RW, D), blk(RW, F), blk(RW, F), blk(RW, F),
                      whole(T, D), whole(T, D), whole(K, T)],
            out_specs=(blk(D, F), blk(D, F), blk(F, D), whole(T, D), whole(T, D), whole(K, T)),
            compiler_params=pltpu.CompilerParams(vmem_limit_bytes=62 * 2 ** 20),
            name="weight_grads",
        )(r, dy, h, da, db, out, gx, gg)
        return out, gx, g1, g3, g2, gg.T

    return jax.shard_map(per_device, mesh=mesh,
                         in_specs=(row_spec, row_spec, row_spec, row_spec, expert_spec, expert_spec, expert_spec, row_spec),
                         out_specs=(row_spec, row_spec, row_spec, row_spec, row_spec, row_spec),
                         check_vma=False)
```

```python
import functools

import jax
import jax.numpy as jnp
from jax import lax
from jax.experimental import pallas as pl
from jax.experimental.pallas import tpu as pltpu
from jax.sharding import PartitionSpec as P

BF16, F32 = jnp.bfloat16, jnp.float32
MESH_ID = pl.DeviceIdType.MESH
LANES = 128
N_CHUNK = 2


def capacity_of(tok_dev, top_k, n_experts):
    return ((2 * tok_dev * top_k + n_experts - 1) // n_experts + 7) // 8 * 8


def dot_nn(a, b):
    return lax.dot_general(a, b, (((1,), (0,)), ((), ())), preferred_element_type=F32)


def dot_nt(a, b):
    return lax.dot_general(a, b, (((1,), (1,)), ((), ())), preferred_element_type=F32)


def dot_tn(a, b):
    return lax.dot_general(a, b, (((0,), (0,)), ((), ())), preferred_element_type=F32)


def moe_kernel(dims, x_hbm, g_hbm, idx_hbm, slot_hbm, gate_hbm, w1_hbm, w3_hbm, w2_hbm,
               w1, w3, w2, out_ref, gx_ref, gg_ref,
               xg, meta, idx_v, slot_v, gate_v, scr, r_all, dy_all, h_all, dab_all, c1_all, c2_all,
               p_all, gs_all, y_all, dr_all, part, sibbuf, ringbuf, finbuf, ggsrc, ggbuf,
               w_sem, loc_sem, meta_ss, meta_rs, ag_ss, ag_rs, rt_ss, rt_rs, gg_ss, gg_rs):
    G, T, D, F, E, C, K = dims
    NQ = G // 2
    RW, NT = G * C, G * T
    CW = D // N_CHUNK
    per_tile = LANES // T
    me = lax.axis_index("ep")
    core = lax.rem(me, 2)
    chip = me // 2
    right_chip, left_chip, opp_chip = (lax.rem(chip + 1, NQ), lax.rem(chip + NQ - 1, NQ), lax.rem(chip + 2, NQ))
    dev = lambda q, c: q * 2 + c
    other = 1 - core
    sib = dev(chip, other)
    right, left, opp = dev(right_chip, core), dev(left_chip, core), dev(opp_chip, core)

    def rows(d):
        return pl.ds(pl.multiple_of(d * T, T), T)

    def remote(src, dst, ss, rs, target):
        return pltpu.make_async_remote_copy(src_ref=src, dst_ref=dst, send_sem=ss, recv_sem=rs,
                                            device_id={"ep": target}, device_id_type=MESH_ID)

    local = [pltpu.make_async_copy(src, dst, loc_sem.at[i]) for i, (src, dst) in enumerate((
        (idx_hbm, idx_v), (slot_hbm, slot_v), (gate_hbm, gate_v),
        (x_hbm, xg.at[0, rows(me)]), (g_hbm, xg.at[1, rows(me)])))]
    barrier = pltpu.get_barrier_semaphore()
    for d in (sib, right, left):
        pl.semaphore_signal(barrier, inc=1, device_id={"ep": d}, device_id_type=MESH_ID)
    scr[...] = jnp.zeros_like(scr)
    for cp in local:
        cp.start()
    for cp in local[:3]:
        cp.wait()
    off = lax.rem(me, per_tile) * T
    scr[0, :, 0:T] = jnp.where(slot_v[...] >= 0, idx_v[...] * C + slot_v[...] + 1, 0).astype(F32)
    scr[1, :, 0:T] = gate_v[...]
    meta[me, 0:K] = pltpu.roll(scr[0], off, 1)
    meta[me, K:2 * K] = pltpu.roll(scr[1], off, 1)
    local[3].wait()
    local[4].wait()
    w_copies = [pltpu.make_async_copy(src.at[e], dst.at[e], w_sem.at[k, e]) for e in range(E)
                for k, (src, dst) in enumerate(((w1_hbm, w1), (w3_hbm, w3), (w2_hbm, w2)))]
    for cp in w_copies:
        cp.start()
    pl.semaphore_wait(barrier, 3)

    lo, hi, full = pl.ds(0, D // 2), pl.ds(D // 2, D // 2), pl.ds(0, D)
    sib_right, sib_left, sib_opp = dev(right_chip, other), dev(left_chip, other), dev(opp_chip, other)
    ag_out = ((me, full, sib), (me, lo, right), (me, hi, right), (me, hi, left), (me, lo, left),
              (left, lo, right), (right, hi, left), (left, full, sib), (right, full, sib),
              (opp, lo, sib), (opp, hi, sib))
    ag_in = ((sib, full, sib), (left, lo, left), (left, hi, left), (right, hi, right), (right, lo, right),
             (opp, lo, left), (opp, hi, right), (sib_left, full, sib), (sib_right, full, sib),
             (sib_opp, lo, sib), (sib_opp, hi, sib))
    meta_out = ((me, sib), (me, right), (me, left), (left, right), (left, sib), (right, sib), (opp, sib))
    meta_in = ((sib, sib), (left, left), (right, right), (opp, left), (sib_left, sib), (sib_right, sib), (sib_opp, sib))

    def ag(table, t, k):
        src_dev, cols, target = table[k]
        ref = xg.at[t, rows(src_dev), cols]
        return remote(ref, ref, ag_ss.at[t, k], ag_rs.at[t, k], target)

    def mt(table, k):
        src_dev, target = table[k]
        return remote(meta.at[src_dev], meta.at[src_dev], meta_ss.at[k], meta_rs.at[k], target)

    def ag_send(t, *ks):
        for k in ks:
            ag(ag_out, t, k).start()

    def ag_recv(t, *ks):
        for k in ks:
            ag(ag_in, t, k).wait_recv()

    def mt_send(*ks):
        for k in ks:
            mt(meta_out, k).start()

    def mt_recv(*ks):
        for k in ks:
            mt(meta_in, k).wait_recv()

    ag_send(0, 1, 3)
    mt_send(1, 2, 0)
    ag_send(0, 2, 4, 0)
    ag_recv(0, 1)
    ag_send(0, 5)
    ag_recv(0, 3)
    ag_send(0, 6)
    mt_recv(1)
    mt_send(3, 4)
    mt_recv(2)
    mt_send(5)
    ag_send(1, 1, 3, 2, 4, 0)
    ag_recv(0, 2)
    ag_send(0, 7)
    ag_recv(0, 4)
    ag_send(0, 8)
    mt_recv(3)
    mt_send(6)
    ag_recv(0, 5)
    ag_send(0, 9)
    ag_recv(0, 6)
    ag_send(0, 10)
    mt_recv(0, 4, 5, 6)

    n_tiles = G // per_tile
    halves = []
    for i in range(n_tiles):
        tot = meta[i * per_tile]
        for s in range(i * per_tile + 1, (i + 1) * per_tile):
            tot = tot + meta[s]
        halves.append(tot)
    codes = jnp.concatenate([v[0:K] for v in halves], axis=1)
    gates = jnp.concatenate([v[K:2 * K] for v in halves], axis=1)
    lane_src = (lax.broadcasted_iota(jnp.int32, (K, NT), 1) // T * C).astype(F32)
    row_id = lax.broadcasted_iota(jnp.int32, (RW, NT), 0).astype(F32) + 1.0

    def routing(e):
        first = ((me * E + e) * C).astype(F32) + 1.0
        sel = (codes >= first) & (codes < first + float(C))
        pos = jnp.sum(jnp.where(sel, codes - first + lane_src + 1.0, 0.0), axis=0, keepdims=True)
        gate_row = jnp.sum(jnp.where(sel, gates, 0.0), axis=0, keepdims=True)
        return sel, row_id == pos, gate_row

    def erow(e):
        return pl.ds(e * RW, RW)

    for e in range(E):
        sel, mask, gate_row = routing(e)
        p_all[erow(e), :] = jnp.where(mask, 1.0, 0.0).astype(BF16)
        rest = gate_row
        for i in range(3):
            piece = rest.astype(BF16).astype(F32)
            gs_all[i, erow(e), :] = jnp.where(mask, piece, 0.0).astype(BF16)
            rest = rest - piece

    ag_recv(0, 0, 7, 8, 9, 10)
    ag_recv(1, 1)
    ag_send(1, 5)
    ag_recv(1, 3)
    ag_send(1, 6)
    for cp in w_copies:
        cp.wait()

    def select_x(e):
        r_all[e] = dot_nn(p_all[erow(e), :], xg[0]).astype(BF16)

    def up(e):
        a = dot_nn(r_all[e], w1[e])
        b = dot_nn(r_all[e], w3[e])
        s = jax.nn.sigmoid(a)
        act = a * s
        h_all[e] = (act * b).astype(BF16)
        c1_all[e] = b * (s * (1.0 + a * (1.0 - s)))
        c2_all[e] = act

    def down(e):
        y_all[erow(e), :] = dot_nn(h_all[e], w2[e]).astype(BF16)

    select_x(0)
    for e in range(E):
        if e + 1 < E:
            select_x(e + 1)
        up(e)
        if e > 0:
            down(e - 1)
        if e == 2:
            ag_recv(1, 2)
            ag_send(1, 7)
            ag_recv(1, 4)
            ag_send(1, 8)
    down(E - 1)
    ag_recv(1, 5)
    ag_send(1, 9)
    ag_recv(1, 6)
    ag_send(1, 10)

    chips = (opp_chip, right_chip, left_chip, chip)
    HW = CW // 2

    def cols(j):
        return pl.ds(j * CW, CW)

    def half(j, i):
        return pl.ds(j * CW + i * HW, HW)

    c_half = (pl.ds(0, HW), pl.ds(HW, HW))

    def ret_desc(t, j, n):
        u = t * N_CHUNK + j
        if n < 4:
            src, dst, tgt = part.at[t, rows(dev(chips[n], other)), cols(j)], sibbuf.at[u, n], sib
        elif n == 4:
            src, dst, tgt = part.at[t, rows(opp), half(j, 0)], ringbuf.at[u, 0], right
        elif n == 5:
            src, dst, tgt = part.at[t, rows(opp), half(j, 1)], ringbuf.at[u, 1], left
        elif n in (6, 8):
            i = 1 if n == 6 else 0
            src, dst, tgt = part.at[t, rows(right), half(j, i)], finbuf.at[u, 0, :, c_half[i]], right
        else:
            i = 0 if n == 7 else 1
            src, dst, tgt = part.at[t, rows(left), half(j, i)], finbuf.at[u, 1, :, c_half[i]], left
        return remote(src, dst, rt_ss.at[u, n], rt_rs.at[u, n], tgt)

    def ret_0(t, j):
        for n in range(4):
            ret_desc(t, j, n).start()

    def ret_1(t, j):
        u = t * N_CHUNK + j
        for n, d in enumerate((opp, right, left, me)):
            ret_desc(t, j, n).wait_recv()
            part[t, rows(d), cols(j)] += sibbuf[u, n]
            for m in ((4, 5), (6,), (7,), ())[n]:
                ret_desc(t, j, m).start()

    def ret_2(t, j):
        u = t * N_CHUNK + j
        for n, d, i in ((4, right, 0), (5, left, 1)):
            ret_desc(t, j, n).wait_recv()
            part[t, rows(d), half(j, i)] += ringbuf[u, i]
            ret_desc(t, j, n + 4).start()

    def ret_3(t, j, res_ref):
        u = t * N_CHUNK + j
        for n in (6, 7, 8, 9):
            ret_desc(t, j, n).wait_recv()
        res_ref[:, cols(j)] = (part[t, rows(me), cols(j)] + finbuf[u, 0] + finbuf[u, 1]).astype(BF16)

    for j in range(N_CHUNK):
        acc = dot_tn(gs_all[0], y_all[:, cols(j)])
        for i in (1, 2):
            acc = acc + dot_tn(gs_all[i], y_all[:, cols(j)])
        part[0, :, cols(j)] = acc
        ret_0(0, j)

    ag_recv(1, 0, 7, 8, 9, 10)

    gg = jnp.zeros((K, NT), F32)

    def select_g(e, gg):
        sel, mask, gate_row = routing(e)
        gate_col = jnp.sum(jnp.where(mask, gate_row, 0.0), axis=1, keepdims=True)
        g_e = dot_nn(p_all[erow(e), :], xg[1])
        dy_all[e] = (gate_col * g_e).astype(BF16)
        gg_col = jnp.sum(g_e * y_all[erow(e), :].astype(F32), axis=1, keepdims=True)
        gg_row = jnp.sum(jnp.where(mask, gg_col, 0.0), axis=0, keepdims=True)
        return gg + jnp.where(sel, gg_row, 0.0)

    def down_t(e):
        dh = dot_nt(dy_all[e], w2[e])
        dab_all[e, :, 0:F] = (dh * c1_all[e]).astype(BF16)
        dab_all[e, :, F:2 * F] = (dh * c2_all[e]).astype(BF16)

    gg = select_g(0, gg)
    for e in range(E):
        if e + 1 < E:
            gg = select_g(e + 1, gg)
        down_t(e)
        if e == 1:
            ret_1(0, 0)
            ret_1(0, 1)
    for i in range(n_tiles):
        ggsrc[i] = gg[:, i * LANES:(i + 1) * LANES]

    def gg_desc(d):
        tgt = lax.rem(me + d, G)
        return remote(ggsrc.at[tgt // per_tile], ggbuf.at[d - 1], gg_ss.at[d - 1], gg_rs.at[d - 1], tgt)

    for j in range(N_CHUNK):
        for e in range(E):
            dr_all[erow(e), cols(j)] = (dot_nt(dab_all[e, :, 0:F], w1[e, cols(j), :])
                                        + dot_nt(dab_all[e, :, F:2 * F], w3[e, cols(j), :])).astype(BF16)
            if e == 1 and j == 0:
                ret_2(0, 0)
                ret_2(0, 1)
            if e == 2 and j > 0:
                ret_1(1, j - 1)
        part[1, :, cols(j)] = dot_tn(p_all[...], dr_all[:, cols(j)])
        ret_0(1, j)

    for d in range(1, G):
        gg_desc(d).start()

    def wgrad(e):
        step = D // 6
        for m in range(6):
            sl = pl.ds(m * step, step)
            res = dot_tn(r_all[e, :, sl], dab_all[e])
            w1[e, sl, :] = res[:, 0:F].astype(BF16)
            w3[e, sl, :] = res[:, F:2 * F].astype(BF16)
        for m in range(2):
            sl = pl.ds(m * (F // 2), F // 2)
            w2[e, sl, :] = dot_tn(h_all[e, :, sl], dy_all[e]).astype(BF16)

    ret_2(1, 0)
    for j in range(N_CHUNK):
        ret_3(0, j, out_ref)
    ret_1(1, N_CHUNK - 1)
    wgrad(0)
    tot = ggsrc[me // per_tile]
    for d in range(1, G):
        gg_desc(d).wait_recv()
        tot = tot + ggbuf[d - 1]
    gg_ref[...] = pltpu.roll(tot, lax.rem(LANES - off, LANES), 1)[:, 0:T]
    wgrad(1)
    ret_2(1, N_CHUNK - 1)
    for e in range(2, E):
        wgrad(e)
    for j in range(N_CHUNK):
        ret_3(1, j, gx_ref)
    for k in range(len(meta_out)):
        mt(meta_out, k).wait_send()
    for t in range(2):
        for k in range(len(ag_out)):
            ag(ag_out, t, k).wait_send()
        for j in range(N_CHUNK):
            for n in range(10):
                ret_desc(t, j, n).wait_send()
    for d in range(1, G):
        gg_desc(d).wait_send()


def write_kernel(n_exp, *refs):
    n = 6
    src, dst, sem = refs[:n], refs[n:2 * n], refs[2 * n]
    copies = []
    for e in range(n_exp):
        for k in range(3):
            copies.append(pltpu.make_async_copy(src[k].at[e], dst[k].at[e], sem.at[k, e]))
    for k in range(3, n):
        copies.append(pltpu.make_async_copy(src[k], dst[k], sem.at[k, 0]))
    for cp in copies:
        cp.start()
    for cp in copies:
        cp.wait()


def solution(mesh):
    group_size = mesh.shape['ep']
    row_spec = P(('dp', 'ep'))
    expert_spec = P('ep')

    def per_device(x_rows, expert_idx, gate_w, slot_pos, w_gate, w_up, w_down, grad_out):
        T, D = x_rows.shape
        K = expert_idx.shape[1]
        E, _, F = w_gate.shape
        G = group_size
        C = capacity_of(T, K, E * G)
        RW, NT = G * C, G * T
        NQ = G // 2
        CW = D // N_CHUNK
        dims = (G, T, D, F, E, C, K)
        vm = pltpu.VMEM
        dma = pltpu.SemaphoreType.DMA
        vspec = pl.BlockSpec(memory_space=pltpu.VMEM)
        aspec = pl.BlockSpec(memory_space=pl.ANY)
        results = [((E, D, F), BF16), ((E, D, F), BF16), ((E, F, D), BF16), ((T, D), BF16), ((T, D), BF16), ((K, T), F32)]
        held = pl.pallas_call(
            functools.partial(moe_kernel, dims),
            out_shape=[vm(*r) for r in results],
            in_specs=[aspec] * 8,
            out_specs=[vspec] * len(results),
            scratch_shapes=[
                vm((2, NT, D), BF16), vm((G, 2 * K, LANES), F32), vm((K, T), jnp.int32), vm((K, T), jnp.int32), vm((K, T), F32),
                vm((2, K, LANES), F32),
                vm((E, RW, D), BF16), vm((E, RW, D), BF16),
                vm((E, RW, F), BF16), vm((E, RW, 2 * F), BF16),
                vm((E, RW, F), F32), vm((E, RW, F), F32),
                vm((E * RW, NT), BF16), vm((3, E * RW, NT), BF16),
                vm((E * RW, D), BF16), vm((E * RW, D), BF16),
                vm((2, NT, D), F32), vm((2 * N_CHUNK, NQ, T, CW), F32),
                vm((2 * N_CHUNK, 2, T, CW // 2), F32), vm((2 * N_CHUNK, 2, T, CW), F32),
                vm((NT // LANES, K, LANES), F32), vm((G - 1, K, LANES), F32),
                dma((3, E)), dma((5,)), dma((7,)), dma((7,)),
                dma((2, 11)), dma((2, 11)), dma((2 * N_CHUNK, 10)), dma((2 * N_CHUNK, 10)),
                dma((G - 1,)), dma((G - 1,)),
            ],
            compiler_params=pltpu.CompilerParams(
                collective_id=0, has_side_effects=True, vmem_limit_bytes=36 * 2 ** 20),
            name="moe_exchange",
        )(x_rows, grad_out, expert_idx.T, slot_pos.T, gate_w.T, w_gate, w_up, w_down)
        g1, g3, g2, out, gx, gg = pl.pallas_call(
            functools.partial(write_kernel, E),
            out_shape=[jax.ShapeDtypeStruct(*r) for r in results],
            in_specs=[vspec] * len(results),
            out_specs=[aspec] * len(results),
            scratch_shapes=[dma((len(results), E))],
            compiler_params=pltpu.CompilerParams(vmem_limit_bytes=2 ** 20),
            name="write_results",
        )(*held)
        return out, gx, g1, g3, g2, gg.T

    return jax.shard_map(per_device, mesh=mesh,
                         in_specs=(row_spec, row_spec, row_spec, row_spec, expert_spec, expert_spec, expert_spec, row_spec),
                         out_specs=(row_spec, row_spec, row_spec, row_spec, row_spec, row_spec),
                         check_vma=False)
```

```python
import functools

import jax
import jax.numpy as jnp
from jax import lax
from jax.experimental import pallas as pl
from jax.experimental.pallas import tpu as pltpu
from jax.sharding import PartitionSpec as P

BF16, F32 = jnp.bfloat16, jnp.float32
MESH_ID = pl.DeviceIdType.MESH
LANES = 128
N_CHUNK = 2
TB = 256
EARLY = 3


def capacity_of(tok_dev, top_k, n_experts):
    return ((2 * tok_dev * top_k + n_experts - 1) // n_experts + 7) // 8 * 8


def dot_nn(a, b):
    return lax.dot_general(a, b, (((1,), (0,)), ((), ())), preferred_element_type=F32)


def dot_nt(a, b):
    return lax.dot_general(a, b, (((1,), (1,)), ((), ())), preferred_element_type=F32)


def dot_tn(a, b):
    return lax.dot_general(a, b, (((0,), (0,)), ((), ())), preferred_element_type=F32)


def up_grads(r, dab, e, g1, g3, n):
    D, F = r.shape[2], dab.shape[2] // 2
    for m in range(0, D, TB):
        sl = pl.ds(m, TB)
        res = dot_tn(r[e, :, sl], dab[e])
        g1[n, sl, :] = res[:, 0:F].astype(BF16)
        g3[n, sl, :] = res[:, F:2 * F].astype(BF16)


def moe_kernel(dims, x_hbm, g_hbm, idx_hbm, slot_hbm, gate_hbm, w1_hbm, w3_hbm, w2_hbm,
               w1, w3, r_all, dy_all, h_all, dab_all, out_ref, gx_ref, gg_ref,
               w2, w13t, xg, meta, idx_v, slot_v, gate_v, scr, tok, c1_all, c2_all,
               p_all, comb, y_all, part, sibbuf, ringbuf, finbuf, ggsrc, ggbuf,
               w_sem, loc_sem, meta_ss, meta_rs, ag_ss, ag_rs, rt_ss, rt_rs, gg_ss, gg_rs):
    G, T, D, F, E, C, K = dims
    NQ = G // 2
    RW, NT = G * C, G * T
    CW = D // N_CHUNK
    per_tile = LANES // T
    me = lax.axis_index("ep")
    core = lax.rem(me, 2)
    chip = me // 2
    right_chip, left_chip, opp_chip = (lax.rem(chip + 1, NQ), lax.rem(chip + NQ - 1, NQ), lax.rem(chip + 2, NQ))
    dev = lambda q, c: q * 2 + c
    other = 1 - core
    sib = dev(chip, other)
    right, left, opp = dev(right_chip, core), dev(left_chip, core), dev(opp_chip, core)

    def rows(d):
        return pl.ds(pl.multiple_of(d * T, T), T)

    def remote(src, dst, ss, rs, target):
        return pltpu.make_async_remote_copy(src_ref=src, dst_ref=dst, send_sem=ss, recv_sem=rs,
                                            device_id={"ep": target}, device_id_type=MESH_ID)

    local = [pltpu.make_async_copy(src, dst, loc_sem.at[i]) for i, (src, dst) in enumerate((
        (idx_hbm, idx_v), (slot_hbm, slot_v), (gate_hbm, gate_v),
        (x_hbm, xg.at[0, rows(me)]), (g_hbm, xg.at[1, rows(me)])))]
    barrier = pltpu.get_barrier_semaphore()
    for d in (sib, right, left):
        pl.semaphore_signal(barrier, inc=1, device_id={"ep": d}, device_id_type=MESH_ID)
    scr[...] = jnp.zeros_like(scr)
    for cp in local:
        cp.start()
    for cp in local[:3]:
        cp.wait()
    off = lax.rem(me, per_tile) * T
    scr[0, :, 0:T] = jnp.where(slot_v[...] >= 0, idx_v[...] * C + slot_v[...] + 1, 0).astype(F32)
    scr[1, :, 0:T] = gate_v[...]
    meta[me, 0:K] = pltpu.roll(scr[0], off, 1)
    meta[me, K:2 * K] = pltpu.roll(scr[1], off, 1)
    local[3].wait()
    local[4].wait()
    w_copies = [pltpu.make_async_copy(src.at[e], dst.at[e], w_sem.at[k, e]) for e in range(E)
                for k, (src, dst) in enumerate(((w1_hbm, w1), (w3_hbm, w3), (w2_hbm, w2)))]
    for cp in w_copies:
        cp.start()
    pl.semaphore_wait(barrier, 3)

    lo, hi, full = pl.ds(0, D // 2), pl.ds(D // 2, D // 2), pl.ds(0, D)
    sib_right, sib_left, sib_opp = dev(right_chip, other), dev(left_chip, other), dev(opp_chip, other)
    ag_out = ((me, full, sib), (me, lo, right), (me, hi, right), (me, hi, left), (me, lo, left),
              (left, lo, right), (right, hi, left), (left, full, sib), (right, full, sib),
              (opp, lo, sib), (opp, hi, sib))
    ag_in = ((sib, full, sib), (left, lo, left), (left, hi, left), (right, hi, right), (right, lo, right),
             (opp, lo, left), (opp, hi, right), (sib_left, full, sib), (sib_right, full, sib),
             (sib_opp, lo, sib), (sib_opp, hi, sib))
    meta_out = ((me, sib), (me, right), (me, left), (left, right), (left, sib), (right, sib), (opp, sib))
    meta_in = ((sib, sib), (left, left), (right, right), (opp, left), (sib_left, sib), (sib_right, sib), (sib_opp, sib))

    def ag(table, t, k):
        src_dev, cols, target = table[k]
        ref = xg.at[t, rows(src_dev), cols]
        return remote(ref, ref, ag_ss.at[t, k], ag_rs.at[t, k], target)

    def mt(table, k):
        src_dev, target = table[k]
        return remote(meta.at[src_dev], meta.at[src_dev], meta_ss.at[k], meta_rs.at[k], target)

    def ag_send(t, *ks):
        for k in ks:
            ag(ag_out, t, k).start()

    def ag_recv(t, *ks):
        for k in ks:
            ag(ag_in, t, k).wait_recv()

    def mt_send(*ks):
        for k in ks:
            mt(meta_out, k).start()

    def mt_recv(*ks):
        for k in ks:
            mt(meta_in, k).wait_recv()

    ag_send(0, 1, 3)
    mt_send(1, 2, 0)
    ag_send(0, 2, 4, 0)
    def wait_w(k, e):
        w_copies[e * 3 + k].wait()

    def flip_up(e):
        wait_w(0, e)
        wait_w(1, e)
        for k, w in enumerate((w1, w3)):
            for i in range(0, D, TB):
                for j in range(0, F, TB):
                    w13t[e, pl.ds(k * F + j, TB), pl.ds(i, TB)] = w[e, pl.ds(i, TB), pl.ds(j, TB)].T

    def flip_down(e):
        for b in range(0, D, F):
            for i in range(0, F, TB):
                for j in range(i, F, TB):
                    up_ref = w2.at[e, pl.ds(i, TB), pl.ds(b + j, TB)]
                    low_ref = w2.at[e, pl.ds(j, TB), pl.ds(b + i, TB)]
                    up_t, low_t = up_ref[...].T, low_ref[...].T
                    up_ref[...] = low_t
                    if i != j:
                        low_ref[...] = up_t

    flip_up(0)
    flip_up(1)
    ag_recv(0, 1)
    ag_send(0, 5)
    ag_recv(0, 3)
    ag_send(0, 6)
    mt_recv(1)
    mt_send(3, 4)
    mt_recv(2)
    mt_send(5)
    ag_send(1, 1, 3, 2, 4, 0)
    flip_up(2)
    ag_recv(0, 2)
    ag_send(0, 7)
    ag_recv(0, 4)
    ag_send(0, 8)
    mt_recv(3)
    mt_send(6)
    flip_up(3)
    flip_up(4)
    ag_recv(0, 5)
    ag_send(0, 9)
    ag_recv(0, 6)
    ag_send(0, 10)
    mt_recv(0, 4, 5, 6)

    n_tiles = G // per_tile
    halves = []
    for i in range(n_tiles):
        tot = meta[i * per_tile]
        for s in range(i * per_tile + 1, (i + 1) * per_tile):
            tot = tot + meta[s]
        halves.append(tot)
    codes = jnp.concatenate([v[0:K] for v in halves], axis=1)
    gates = jnp.concatenate([v[K:2 * K] for v in halves], axis=1)
    lane_src = (lax.broadcasted_iota(jnp.int32, (K, NT), 1) // T * C).astype(F32)
    row_id = lax.broadcasted_iota(jnp.int32, (RW, NT), 0).astype(F32) + 1.0

    def routing(e):
        first = ((me * E + e) * C).astype(F32) + 1.0
        sel = (codes >= first) & (codes < first + float(C))
        pos = jnp.sum(jnp.where(sel, codes - first + lane_src + 1.0, 0.0), axis=0, keepdims=True)
        gate_row = jnp.sum(jnp.where(sel, gates, 0.0), axis=0, keepdims=True)
        return sel, row_id == pos, gate_row

    def erow(e):
        return pl.ds(e * RW, RW)

    for e in range(E):
        p_all[erow(e), :] = jnp.where(routing(e)[1], 1.0, 0.0).astype(BF16)

    EC = E * C
    tok[...] = jnp.transpose(jnp.concatenate([codes, gates], axis=0))
    pair = lax.broadcasted_iota(jnp.int32, (NT, LANES), 1)
    want = jnp.where(pair < EC, pair + me * EC + 1, -1).astype(F32)
    one, rest = jnp.zeros((NT, LANES), F32), jnp.zeros((NT, LANES), F32)
    for k in range(K):
        hit = tok[:, k:k + 1] == want
        one = jnp.where(hit, 1.0, one)
        rest = jnp.where(hit, tok[:, K + k:K + k + 1], rest)
    for i in range(3):
        piece = rest.astype(BF16)
        for s in range(G):
            comb[s, pl.ds(i * T, T), :] = piece[s * T:(s + 1) * T]
        rest = rest - piece.astype(F32)
    for s in range(G):
        comb[s, pl.ds(3 * T, T), :] = one[s * T:(s + 1) * T].astype(BF16)

    ag_recv(0, 0, 7, 8, 9, 10)
    ag_recv(1, 1)
    ag_send(1, 5)
    ag_recv(1, 3)
    ag_send(1, 6)
    for e in range(E):
        wait_w(2, e)

    def select_x(e):
        r_all[e] = dot_nn(p_all[erow(e), :], xg[0]).astype(BF16)

    def up(e):
        a = dot_nn(r_all[e], w1[e])
        b = dot_nn(r_all[e], w3[e])
        s = jax.nn.sigmoid(a)
        act = a * s
        h_all[e] = (act * b).astype(BF16)
        c1_all[e] = b * (s * (1.0 + a * (1.0 - s)))
        c2_all[e] = act

    select_x(0)
    for e in range(E):
        if e + 1 < E:
            select_x(e + 1)
        up(e)
        if e == 2:
            ag_recv(1, 2)
            ag_send(1, 7)
            ag_recv(1, 4)
            ag_send(1, 8)

    chips = (opp_chip, right_chip, left_chip, chip)
    HW = CW // 2

    def cols(j):
        return pl.ds(j * CW, CW)

    def half(j, i):
        return pl.ds(j * CW + i * HW, HW)

    c_half = (pl.ds(0, HW), pl.ds(HW, HW))

    def ret_desc(t, j, n):
        u = t * N_CHUNK + j
        if n < 4:
            src, dst, tgt = part.at[t, rows(dev(chips[n], other)), cols(j)], sibbuf.at[u, n], sib
        elif n == 4:
            src, dst, tgt = part.at[t, rows(opp), half(j, 0)], ringbuf.at[u, 0], right
        elif n == 5:
            src, dst, tgt = part.at[t, rows(opp), half(j, 1)], ringbuf.at[u, 1], left
        elif n in (6, 8):
            i = 1 if n == 6 else 0
            src, dst, tgt = part.at[t, rows(right), half(j, i)], finbuf.at[u, 0, :, c_half[i]], right
        else:
            i = 0 if n == 7 else 1
            src, dst, tgt = part.at[t, rows(left), half(j, i)], finbuf.at[u, 1, :, c_half[i]], left
        return remote(src, dst, rt_ss.at[u, n], rt_rs.at[u, n], tgt)

    def ret_0(t, j):
        for n in range(4):
            ret_desc(t, j, n).start()

    def ret_1(t, j):
        u = t * N_CHUNK + j
        for n, d in enumerate((opp, right, left, me)):
            ret_desc(t, j, n).wait_recv()
            part[t, rows(d), cols(j)] += sibbuf[u, n]
            for m in ((4, 5), (6,), (7,), ())[n]:
                ret_desc(t, j, m).start()

    def ret_2(t, j):
        u = t * N_CHUNK + j
        for n, d, i in ((4, right, 0), (5, left, 1)):
            ret_desc(t, j, n).wait_recv()
            part[t, rows(d), half(j, i)] += ringbuf[u, i]
            ret_desc(t, j, n + 4).start()

    def ret_3(t, j, res_ref):
        u = t * N_CHUNK + j
        for n in (6, 7, 8, 9):
            ret_desc(t, j, n).wait_recv()
        res_ref[:, cols(j)] = (part[t, rows(me), cols(j)] + finbuf[u, 0] + finbuf[u, 1]).astype(BF16)

    def put_rows(e, j, val):
        for s in range(G):
            y_all[s, pl.ds(e * C, C), cols(j)] = val[s * C:(s + 1) * C]

    for j in range(N_CHUNK):
        for e in range(E):
            put_rows(e, j, dot_nn(h_all[e], w2[e, :, cols(j)]).astype(BF16))
        for s in range(G):
            acc = dot_nn(comb[s, 0:3 * T, 0:EC], y_all[s, :, cols(j)])
            part[0, pl.ds(s * T, T), cols(j)] = acc[0:T] + acc[T:2 * T] + acc[2 * T:3 * T]
        ret_0(0, j)
        if j == 0:
            ag_recv(1, 5)
            ag_send(1, 9)
            ag_recv(1, 6)
            ag_send(1, 10)

    ag_recv(1, 0, 7, 8, 9, 10)

    gg = jnp.zeros((K, NT), F32)

    def select_g(e, gg):
        sel, mask, gate_row = routing(e)
        gate_col = jnp.sum(jnp.where(mask, gate_row, 0.0), axis=1, keepdims=True)
        g_e = dot_nn(p_all[erow(e), :], xg[1])
        dy_all[e] = (gate_col * g_e).astype(BF16)
        y_e = y_all[:, pl.ds(e * C, C), :].reshape(RW, D)
        gg_col = jnp.sum(g_e * y_e.astype(F32), axis=1, keepdims=True)
        gg_row = jnp.sum(jnp.where(mask, gg_col, 0.0), axis=0, keepdims=True)
        return gg + jnp.where(sel, gg_row, 0.0)

    def down_t(e):
        dh = dot_nn(dy_all[e, :, 0:F], w2[e, :, 0:F])
        for b in range(F, D, F):
            dh = dh + dot_nn(dy_all[e, :, b:b + F], w2[e, :, b:b + F])
        dab_all[e, :, 0:F] = (dh * c1_all[e]).astype(BF16)
        dab_all[e, :, F:2 * F] = (dh * c2_all[e]).astype(BF16)

    flip_down(0)
    gg = select_g(0, gg)
    for e in range(E):
        if e + 1 < E:
            flip_down(e + 1)
            gg = select_g(e + 1, gg)
        down_t(e)
        if e == 2:
            ret_1(0, 0)
            ret_1(0, 1)
    for i in range(n_tiles):
        ggsrc[i] = gg[:, i * LANES:(i + 1) * LANES]

    def gg_desc(d):
        tgt = lax.rem(me + d, G)
        return remote(ggsrc.at[tgt // per_tile], ggbuf.at[d - 1], gg_ss.at[d - 1], gg_rs.at[d - 1], tgt)

    for j in range(N_CHUNK):
        for e in range(E):
            put_rows(e, j, dot_nn(dab_all[e], w13t[e, :, cols(j)]).astype(BF16))
            if e == 2 and j > 0:
                ret_1(1, j - 1)
        for s in range(G):
            part[1, pl.ds(s * T, T), cols(j)] = dot_nn(comb[s, 3 * T:4 * T, 0:EC], y_all[s, :, cols(j)])
        ret_0(1, j)
        if j == 0:
            ret_2(0, 0)
            ret_2(0, 1)

    for d in range(1, G):
        gg_desc(d).start()

    ret_2(1, 0)
    for j in range(N_CHUNK):
        ret_3(0, j, out_ref)
    ret_1(1, N_CHUNK - 1)
    up_grads(r_all, dab_all, 0, w1, w3, 0)
    tot = ggsrc[me // per_tile]
    for d in range(1, G):
        gg_desc(d).wait_recv()
        tot = tot + ggbuf[d - 1]
    gg_ref[...] = pltpu.roll(tot, lax.rem(LANES - off, LANES), 1)[:, 0:T]
    up_grads(r_all, dab_all, 1, w1, w3, 1)
    ret_2(1, N_CHUNK - 1)
    for e in range(2, EARLY):
        up_grads(r_all, dab_all, e, w1, w3, e)
    for j in range(N_CHUNK):
        ret_3(1, j, gx_ref)
    for k in range(len(meta_out)):
        mt(meta_out, k).wait_send()
    for t in range(2):
        for k in range(len(ag_out)):
            ag(ag_out, t, k).wait_send()
        for j in range(N_CHUNK):
            for n in range(10):
                ret_desc(t, j, n).wait_send()
    for d in range(1, G):
        gg_desc(d).wait_send()


def write_kernel(n_exp, g1, g3, r, dy, h, dab, out, gx, gg, g1_hbm, g3_hbm, g2_hbm, out_hbm, gx_hbm, gg_hbm,
                 late1, late3, g2, sem, small_sem):
    copies = []

    def send(src, dst, s):
        copies.append(pltpu.make_async_copy(src, dst, s))
        copies[-1].start()

    for e in range(EARLY):
        send(g1.at[e], g1_hbm.at[e], sem.at[0, e])
        send(g3.at[e], g3_hbm.at[e], sem.at[1, e])
    for k, (src, dst) in enumerate(((out, out_hbm), (gx, gx_hbm), (gg, gg_hbm))):
        send(src, dst, small_sem.at[k])
    F = h.shape[2]
    for e in range(n_exp):
        for m in range(0, F, TB):
            g2[e, pl.ds(m, TB), :] = dot_tn(h[e, :, pl.ds(m, TB)], dy[e]).astype(BF16)
        send(g2.at[e], g2_hbm.at[e], sem.at[2, e])
        if e >= EARLY:
            n = e - EARLY
            up_grads(r, dab, e, late1, late3, n)
            send(late1.at[n], g1_hbm.at[e], sem.at[0, e])
            send(late3.at[n], g3_hbm.at[e], sem.at[1, e])
    for cp in copies:
        cp.wait()


def solution(mesh):
    group_size = mesh.shape['ep']
    row_spec = P(('dp', 'ep'))
    expert_spec = P('ep')

    def per_device(x_rows, expert_idx, gate_w, slot_pos, w_gate, w_up, w_down, grad_out):
        T, D = x_rows.shape
        K = expert_idx.shape[1]
        E, _, F = w_gate.shape
        G = group_size
        C = capacity_of(T, K, E * G)
        RW, NT = G * C, G * T
        NQ = G // 2
        CW = D // N_CHUNK
        dims = (G, T, D, F, E, C, K)
        vm = pltpu.VMEM
        dma = pltpu.SemaphoreType.DMA
        vspec = pl.BlockSpec(memory_space=pltpu.VMEM)
        aspec = pl.BlockSpec(memory_space=pl.ANY)
        small = [((T, D), BF16), ((T, D), BF16), ((K, T), F32)]
        held_shapes = [((E, D, F), BF16), ((E, D, F), BF16), ((E, RW, D), BF16), ((E, RW, D), BF16),
                       ((E, RW, F), BF16), ((E, RW, 2 * F), BF16)] + small
        results = [((E, D, F), BF16), ((E, D, F), BF16), ((E, F, D), BF16)] + small
        n_units = 2 * N_CHUNK
        held = pl.pallas_call(
            functools.partial(moe_kernel, dims),
            out_shape=[vm(*r) for r in held_shapes],
            in_specs=[aspec] * 8,
            out_specs=[vspec] * len(held_shapes),
            scratch_shapes=[
                vm((E, F, D), BF16), vm((E, 2 * F, D), BF16),
                vm((2, NT, D), BF16), vm((G, 2 * K, LANES), F32),
                vm((K, T), jnp.int32), vm((K, T), jnp.int32), vm((K, T), F32),
                vm((2, K, LANES), F32), vm((NT, 2 * K), F32),
                vm((E, RW, F), F32), vm((E, RW, F), F32),
                vm((E * RW, NT), BF16), vm((G, 4 * T, LANES), BF16),
                vm((G, E * C, D), BF16),
                vm((2, NT, D), F32), vm((n_units, NQ, T, CW), F32),
                vm((n_units, 2, T, CW // 2), F32), vm((n_units, 2, T, CW), F32),
                vm((NT // LANES, K, LANES), F32), vm((G - 1, K, LANES), F32),
                dma((3, E)), dma((5,)), dma((7,)), dma((7,)),
                dma((2, 11)), dma((2, 11)), dma((n_units, 10)), dma((n_units, 10)),
                dma((G - 1,)), dma((G - 1,)),
            ],
            compiler_params=pltpu.CompilerParams(
                collective_id=0, has_side_effects=True, vmem_limit_bytes=39 * 2 ** 20),
            name="moe_exchange",
        )(x_rows, grad_out, expert_idx.T, slot_pos.T, gate_w.T, w_gate, w_up, w_down)
        g1, g3, g2, out, gx, gg = pl.pallas_call(
            functools.partial(write_kernel, E),
            out_shape=[jax.ShapeDtypeStruct(*r) for r in results],
            in_specs=[vspec] * len(held_shapes),
            out_specs=[aspec] * len(results),
            scratch_shapes=[vm((E - EARLY, D, F), BF16), vm((E - EARLY, D, F), BF16), vm((E, F, D), BF16),
                            dma((3, E)), dma((len(small),))],
            compiler_params=pltpu.CompilerParams(vmem_limit_bytes=16 * 2 ** 20),
            name="write_results",
        )(*held)
        return out, gx, g1, g3, g2, gg.T

    return jax.shard_map(per_device, mesh=mesh,
                         in_specs=(row_spec, row_spec, row_spec, row_spec, expert_spec, expert_spec, expert_spec, row_spec),
                         out_specs=(row_spec, row_spec, row_spec, row_spec, row_spec, row_spec),
                         check_vma=False)
```

```python
import functools

import jax
import jax.numpy as jnp
from jax import lax
from jax.experimental import pallas as pl
from jax.experimental.pallas import tpu as pltpu
from jax.sharding import PartitionSpec as P

BF16, F32 = jnp.bfloat16, jnp.float32
MESH_ID = pl.DeviceIdType.MESH
LANES = 128
N_CHUNK = 3
TB = 256
EARLY = 4


def capacity_of(tok_dev, top_k, n_experts):
    return ((2 * tok_dev * top_k + n_experts - 1) // n_experts + 7) // 8 * 8


def dot_nn(a, b):
    return lax.dot_general(a, b, (((1,), (0,)), ((), ())), preferred_element_type=F32)


def dot_nt(a, b):
    return lax.dot_general(a, b, (((1,), (1,)), ((), ())), preferred_element_type=F32)


def dot_tn(a, b):
    return lax.dot_general(a, b, (((0,), (0,)), ((), ())), preferred_element_type=F32)


def up_grads(r, dab, e, g1, g3, n):
    D, F = r.shape[2], dab.shape[2] // 2
    for m in range(0, D, TB):
        sl = pl.ds(m, TB)
        res = dot_tn(r[e, :, sl], dab[e])
        g1[n, sl, :] = res[:, 0:F].astype(BF16)
        g3[n, sl, :] = res[:, F:2 * F].astype(BF16)


def moe_kernel(dims, x_hbm, g_hbm, idx_hbm, slot_hbm, gate_hbm, w1_hbm, w3_hbm, w2_hbm,
               w1, w3, r_all, dy_all, h_all, dab_all, out_ref, gx_ref, gg_ref,
               w2, w1t, w2t, xg, meta, idx_v, slot_v, gate_v, scr, tok, c1_all, c2_all,
               p_all, comb, y_all, part, sibbuf, ringbuf, finbuf, ggsrc, ggbuf,
               w_sem, loc_sem, meta_ss, meta_rs, ag_ss, ag_rs, rt_ss, rt_rs, gg_sem):
    G, T, D, F, E, C, K = dims
    NQ = G // 2
    RW, NT = G * C, G * T
    CW = D // N_CHUNK
    assert CW == F and G == 8
    per_tile = LANES // T
    me = lax.axis_index("ep")
    core = lax.rem(me, 2)
    chip = me // 2
    right_chip, left_chip, opp_chip = (lax.rem(chip + 1, NQ), lax.rem(chip + NQ - 1, NQ), lax.rem(chip + 2, NQ))
    dev = lambda q, c: q * 2 + c
    other = 1 - core
    sib = dev(chip, other)
    right, left, opp = dev(right_chip, core), dev(left_chip, core), dev(opp_chip, core)

    def rows(d):
        return pl.ds(pl.multiple_of(d * T, T), T)

    def remote(src, dst, ss, rs, target):
        return pltpu.make_async_remote_copy(src_ref=src, dst_ref=dst, send_sem=ss, recv_sem=rs,
                                            device_id={"ep": target}, device_id_type=MESH_ID)

    local = [pltpu.make_async_copy(src, dst, loc_sem.at[i]) for i, (src, dst) in enumerate((
        (idx_hbm, idx_v), (slot_hbm, slot_v), (gate_hbm, gate_v),
        (x_hbm, xg.at[0, rows(me)]), (g_hbm, xg.at[1, rows(me)])))]

    def wait_bytes(ref, sem):
        pltpu.make_async_copy(ref, ref, sem).wait()

    barrier = pltpu.get_barrier_semaphore()
    for d in (sib, right, left):
        pl.semaphore_signal(barrier, inc=1, device_id={"ep": d}, device_id_type=MESH_ID)
    scr[...] = jnp.zeros_like(scr)
    for cp in local:
        cp.start()
    for cp in local[:3]:
        cp.wait()
    off = lax.rem(me, per_tile) * T
    scr[0, :, 0:T] = jnp.where(slot_v[...] >= 0, idx_v[...] * C + slot_v[...] + 1, 0).astype(F32)
    scr[1, :, 0:T] = gate_v[...]
    meta[me, 0:K] = pltpu.roll(scr[0], off, 1)
    meta[me, K:2 * K] = pltpu.roll(scr[1], off, 1)
    local[3].wait()
    local[4].wait()
    for e in range(E):
        pltpu.make_async_copy(w1_hbm.at[e], w1.at[e], w_sem.at[e]).start()
        pltpu.make_async_copy(w2_hbm.at[e], w2.at[e], w_sem.at[e]).start()
    for e in range(E):
        pltpu.make_async_copy(w3_hbm.at[e], w3.at[e], w_sem.at[E]).start()
    pl.semaphore_wait(barrier, 3)

    lo, hi, full = pl.ds(0, D // 2), pl.ds(D // 2, D // 2), pl.ds(0, D)
    sib_right, sib_left, sib_opp = dev(right_chip, other), dev(left_chip, other), dev(opp_chip, other)
    ag_out = ((me, full, sib), (me, lo, right), (me, hi, right), (me, hi, left), (me, lo, left),
              (left, lo, right), (right, hi, left), (left, full, sib), (right, full, sib),
              (opp, lo, sib), (opp, hi, sib))
    ag_in = ((sib, full, sib), (left, lo, left), (left, hi, left), (right, hi, right), (right, lo, right),
             (opp, lo, left), (opp, hi, right), (sib_left, full, sib), (sib_right, full, sib),
             (sib_opp, lo, sib), (sib_opp, hi, sib))
    meta_out = ((me, sib), (me, right), (me, left), (left, right), (left, sib), (right, sib), (opp, sib))
    meta_in = ((sib, sib), (left, left), (right, right), (opp, left), (sib_left, sib), (sib_right, sib), (sib_opp, sib))

    def ag(table, t, k):
        src_dev, cols, target = table[k]
        ref = xg.at[t, rows(src_dev), cols]
        return remote(ref, ref, ag_ss.at[t], ag_rs.at[t, k if k < 7 else 0], target)

    def mt(table, k):
        src_dev, target = table[k]
        return remote(meta.at[src_dev], meta.at[src_dev], meta_ss, meta_rs.at[k if k < 4 else 0], target)

    def ag_send(t, *ks):
        for k in ks:
            ag(ag_out, t, k).start()

    def ag_recv(t, *ks):
        for k in ks:
            ag(ag_in, t, k).wait_recv()

    def ag_recv_sib(t):
        wait_bytes(xg.at[t, pl.ds(0, NQ * T)], ag_rs.at[t, 0])

    def mt_send(*ks):
        for k in ks:
            mt(meta_out, k).start()

    def mt_recv(*ks):
        for k in ks:
            mt(meta_in, k).wait_recv()

    ag_send(0, 1, 3)
    mt_send(1, 2, 0)
    ag_send(0, 2, 4, 0)

    def flip(dst, src):
        for i in range(0, src.shape[0], TB):
            for j in range(0, src.shape[1], TB):
                dst[pl.ds(j, TB), pl.ds(i, TB)] = src[pl.ds(i, TB), pl.ds(j, TB)].T

    def flip_12(e):
        wait_bytes(w1.at[pl.ds(0, 2)], w_sem.at[e])
        flip(w1t.at[e], w1.at[e])
        flip(w2t.at[e], w2.at[e])

    def flip_3(e):
        for b in range(0, D, F):
            for i in range(0, F, TB):
                for j in range(i, F, TB):
                    up_ref = w3.at[e, pl.ds(b + i, TB), pl.ds(j, TB)]
                    low_ref = w3.at[e, pl.ds(b + j, TB), pl.ds(i, TB)]
                    up_t, low_t = up_ref[...].T, low_ref[...].T
                    up_ref[...] = low_t
                    if i != j:
                        low_ref[...] = up_t

    flip_12(0)
    ag_recv(0, 1)
    ag_send(0, 5)
    ag_recv(0, 3)
    ag_send(0, 6)
    mt_recv(1)
    mt_send(3, 4)
    mt_recv(2)
    mt_send(5)
    ag_send(1, 1, 3, 2, 4, 0)
    flip_12(1)
    flip_12(2)
    ag_recv(0, 2)
    ag_send(0, 7)
    ag_recv(0, 4)
    ag_send(0, 8)
    mt_recv(3)
    mt_send(6)
    flip_12(3)
    ag_recv(0, 5)
    ag_send(0, 9)
    ag_recv(0, 6)
    ag_send(0, 10)
    flip_12(E - 1)
    wait_bytes(meta.at[pl.ds(0, NQ)], meta_rs.at[0])

    n_tiles = G // per_tile
    halves = []
    for i in range(n_tiles):
        tot = meta[i * per_tile]
        for s in range(i * per_tile + 1, (i + 1) * per_tile):
            tot = tot + meta[s]
        halves.append(tot)
    codes = jnp.concatenate([v[0:K] for v in halves], axis=1)
    gates = jnp.concatenate([v[K:2 * K] for v in halves], axis=1)
    lane_src = (lax.broadcasted_iota(jnp.int32, (K, NT), 1) // T * C).astype(F32)
    row_id = lax.broadcasted_iota(jnp.int32, (RW, NT), 0).astype(F32) + 1.0

    def routing(e):
        first = ((me * E + e) * C).astype(F32) + 1.0
        sel = (codes >= first) & (codes < first + float(C))
        pos = jnp.sum(jnp.where(sel, codes - first + lane_src + 1.0, 0.0), axis=0, keepdims=True)
        gate_row = jnp.sum(jnp.where(sel, gates, 0.0), axis=0, keepdims=True)
        return sel, row_id == pos, gate_row

    def erow(e):
        return pl.ds(e * RW, RW)

    for e in range(E):
        p_all[erow(e), :] = jnp.where(routing(e)[1], 1.0, 0.0).astype(BF16)

    EC = E * C

    def build_comb():
        tok[...] = jnp.transpose(jnp.concatenate([codes, gates], axis=0))
        pair = lax.broadcasted_iota(jnp.int32, (NT, LANES), 1)
        want = jnp.where(pair < EC, pair + me * EC + 1, -1).astype(F32)
        one, rest = jnp.zeros((NT, LANES), F32), jnp.zeros((NT, LANES), F32)
        for k in range(K):
            hit = tok[:, k:k + 1] == want
            one = jnp.where(hit, 1.0, one)
            rest = jnp.where(hit, tok[:, K + k:K + k + 1], rest)
        for i in range(3):
            piece = rest.astype(BF16)
            for s in range(G):
                comb[s, pl.ds(i * T, T), :] = piece[s * T:(s + 1) * T]
            rest = rest - piece.astype(F32)
        for s in range(G):
            comb[s, pl.ds(3 * T, T), :] = one[s * T:(s + 1) * T].astype(BF16)

    ag_recv_sib(0)
    wait_bytes(w3, w_sem.at[E])

    ag_recv(1, 1)
    ag_send(1, 5)
    ag_recv(1, 3)
    ag_send(1, 6)

    def select_x(e):
        r_all[e] = dot_nn(p_all[erow(e), :], xg[0]).astype(BF16)

    def up(e):
        a = dot_nn(r_all[e], w1[e])
        b = dot_nn(r_all[e], w3[e])
        s = jax.nn.sigmoid(a)
        act = a * s
        h_all[e] = (act * b).astype(BF16)
        c1_all[e] = b * (s * (1.0 + a * (1.0 - s)))
        c2_all[e] = act

    select_x(0)
    for e in range(E):
        if e + 1 < E:
            select_x(e + 1)
        up(e)
        flip_3(e)
        if e == 0:
            build_comb()
        if e == 2:
            ag_recv(1, 2)
            ag_send(1, 7)
            ag_recv(1, 4)
            ag_send(1, 8)

    chips = (opp_chip, right_chip, left_chip, chip)
    HW = CW // 2

    def cols(j):
        return pl.ds(j * CW, CW)

    def half(j, i):
        return pl.ds(j * CW + i * HW, HW)

    c_half = (pl.ds(0, HW), pl.ds(HW, HW))

    def ret_desc(t, j, n):
        u = t * N_CHUNK + j
        if n < 4:
            src, dst, tgt = part.at[t, rows(dev(chips[n], other)), cols(j)], sibbuf.at[u, n], sib
        elif n == 4:
            src, dst, tgt = part.at[t, rows(opp), half(j, 0)], ringbuf.at[u, 0], right
        elif n == 5:
            src, dst, tgt = part.at[t, rows(opp), half(j, 1)], ringbuf.at[u, 1], left
        elif n in (6, 8):
            i = 1 if n == 6 else 0
            src, dst, tgt = part.at[t, rows(right), half(j, i)], finbuf.at[u, 0, :, c_half[i]], right
        else:
            i = 0 if n == 7 else 1
            src, dst, tgt = part.at[t, rows(left), half(j, i)], finbuf.at[u, 1, :, c_half[i]], left
        return remote(src, dst, rt_ss, rt_rs.at[u, (0, 0, 0, 0, 1, 2, 3, 4, 3, 4)[n]], tgt)

    def ret_0(t, j):
        for n in range(4):
            ret_desc(t, j, n).start()

    def ret_1(t, j):
        u = t * N_CHUNK + j
        wait_bytes(sibbuf.at[u], rt_rs.at[u, 0])
        for n, d in enumerate((opp, right, left, me)):
            part[t, rows(d), cols(j)] += sibbuf[u, n]
            for m in ((4, 5), (6,), (7,), ())[n]:
                ret_desc(t, j, m).start()

    def ret_2(t, j):
        u = t * N_CHUNK + j
        for n, d, i in ((4, right, 0), (5, left, 1)):
            ret_desc(t, j, n).wait_recv()
            part[t, rows(d), half(j, i)] += ringbuf[u, i]
            ret_desc(t, j, n + 4).start()

    def ret_3(t, j, res_ref):
        u = t * N_CHUNK + j
        wait_bytes(finbuf.at[u, 0], rt_rs.at[u, 3])
        wait_bytes(finbuf.at[u, 1], rt_rs.at[u, 4])
        res_ref[:, cols(j)] = (part[t, rows(me), cols(j)] + finbuf[u, 0] + finbuf[u, 1]).astype(BF16)

    def put_rows(e, j, val):
        for s in range(G):
            y_all[s, pl.ds(e * C, C), cols(j)] = val[s * C:(s + 1) * C]

    for j in range(N_CHUNK):
        for e in range(E):
            put_rows(e, j, dot_nn(h_all[e], w2[e, :, cols(j)]).astype(BF16))
        for s in range(G):
            acc = dot_nn(comb[s, 0:3 * T, 0:EC], y_all[s, :, cols(j)])
            part[0, pl.ds(s * T, T), cols(j)] = acc[0:T] + acc[T:2 * T] + acc[2 * T:3 * T]
        ret_0(0, j)
        if j == 0:
            ag_recv(1, 5)
            ag_send(1, 9)
            ag_recv(1, 6)
            ag_send(1, 10)

    ag_recv_sib(1)

    gg = jnp.zeros((K, NT), F32)

    def select_g(e, gg):
        sel, mask, gate_row = routing(e)
        gate_col = jnp.sum(jnp.where(mask, gate_row, 0.0), axis=1, keepdims=True)
        g_e = dot_nn(p_all[erow(e), :], xg[1])
        dy_all[e] = (gate_col * g_e).astype(BF16)
        y_e = y_all[:, pl.ds(e * C, C), :].reshape(RW, D)
        gg_col = jnp.sum(g_e * y_e.astype(F32), axis=1, keepdims=True)
        gg_row = jnp.sum(jnp.where(mask, gg_col, 0.0), axis=0, keepdims=True)
        return gg + jnp.where(sel, gg_row, 0.0)

    def down_t(e):
        dh = dot_nn(dy_all[e], w2t[e])
        dab_all[e, :, 0:F] = (dh * c1_all[e]).astype(BF16)
        dab_all[e, :, F:2 * F] = (dh * c2_all[e]).astype(BF16)

    gg = select_g(0, gg)
    for e in range(E):
        if e + 1 < E:
            gg = select_g(e + 1, gg)
        down_t(e)
        if e < N_CHUNK:
            ret_1(0, e)
    for i in range(n_tiles):
        ggsrc[i] = gg[:, i * LANES:(i + 1) * LANES]

    def gg_desc(d):
        tgt = lax.rem(me + d, G)
        return remote(ggsrc.at[tgt // per_tile], ggbuf.at[d - 1], gg_sem.at[0], gg_sem.at[1], tgt)

    for j in range(N_CHUNK):
        for e in range(E):
            dr = dot_nn(dab_all[e, :, 0:F], w1t[e, :, cols(j)]) + dot_nn(dab_all[e, :, F:2 * F], w3[e, cols(j), :])
            put_rows(e, j, dr.astype(BF16))
        if j == 2:
            ret_1(1, 0)
        for s in range(G):
            part[1, pl.ds(s * T, T), cols(j)] = dot_nn(comb[s, 3 * T:4 * T, 0:EC], y_all[s, :, cols(j)])
        ret_0(1, j)
        ret_2(0, j)

    for d in range(1, G):
        gg_desc(d).start()

    ret_1(1, 1)
    up_grads(r_all, dab_all, 0, w1, w3, 0)
    ret_1(1, 2)
    up_grads(r_all, dab_all, 1, w1, w3, 1)
    ret_2(1, 0)
    ret_2(1, 1)
    up_grads(r_all, dab_all, 2, w1, w3, 2)
    ret_2(1, 2)
    for j in range(N_CHUNK):
        ret_3(0, j, out_ref)
    for e in range(3, EARLY):
        up_grads(r_all, dab_all, e, w1, w3, e)
    tot = ggsrc[me // per_tile]
    wait_bytes(ggbuf, gg_sem.at[1])
    for d in range(1, G):
        tot = tot + ggbuf[d - 1]
    gg_ref[...] = pltpu.roll(tot, lax.rem(LANES - off, LANES), 1)[:, 0:T]
    for j in range(N_CHUNK):
        ret_3(1, j, gx_ref)
    sent = pl.ds(0, (G - 1) * T)
    wait_bytes(meta.at[pl.ds(0, G - 1)], meta_ss)
    wait_bytes(xg.at[0, sent], ag_ss.at[0])
    wait_bytes(xg.at[1, sent], ag_ss.at[1])
    wait_bytes(ggbuf, gg_sem.at[0])
    wait_bytes(part.at[:, sent], rt_ss)


def write_kernel(n_exp, g1, g3, r, dy, h, dab, out, gx, gg, g1_hbm, g3_hbm, g2_hbm, out_hbm, gx_hbm, gg_hbm,
                 late1, late3, g2, sem):
    def send(src, dst, k):
        pltpu.make_async_copy(src, dst, sem.at[k]).start()

    for e in range(EARLY):
        send(g1.at[e], g1_hbm.at[e], 0)
        send(g3.at[e], g3_hbm.at[e], 1)
    for k, (src, dst) in enumerate(((out, out_hbm), (gx, gx_hbm), (gg, gg_hbm))):
        send(src, dst, 3 + k)
    F = h.shape[2]
    for e in range(n_exp):
        for m in range(0, F, TB):
            g2[e, pl.ds(m, TB), :] = dot_tn(h[e, :, pl.ds(m, TB)], dy[e]).astype(BF16)
        send(g2.at[e], g2_hbm.at[e], 2)
        if e >= EARLY:
            n = e - EARLY
            up_grads(r, dab, e, late1, late3, n)
            send(late1.at[n], g1_hbm.at[e], 0)
            send(late3.at[n], g3_hbm.at[e], 1)
    for k, ref in enumerate((g1_hbm, g3_hbm, g2_hbm, out_hbm, gx_hbm, gg_hbm)):
        pltpu.make_async_copy(ref, ref, sem.at[k]).wait()


def solution(mesh):
    group_size = mesh.shape['ep']
    row_spec = P(('dp', 'ep'))
    expert_spec = P('ep')

    def per_device(x_rows, expert_idx, gate_w, slot_pos, w_gate, w_up, w_down, grad_out):
        T, D = x_rows.shape
        K = expert_idx.shape[1]
        E, _, F = w_gate.shape
        G = group_size
        C = capacity_of(T, K, E * G)
        RW, NT = G * C, G * T
        NQ = G // 2
        CW = D // N_CHUNK
        dims = (G, T, D, F, E, C, K)
        vm = pltpu.VMEM
        dma = pltpu.SemaphoreType.DMA
        vspec = pl.BlockSpec(memory_space=pltpu.VMEM)
        aspec = pl.BlockSpec(memory_space=pl.ANY)
        small = [((T, D), BF16), ((T, D), BF16), ((K, T), F32)]
        held_shapes = [((E, D, F), BF16), ((E, D, F), BF16), ((E, RW, D), BF16), ((E, RW, D), BF16),
                       ((E, RW, F), BF16), ((E, RW, 2 * F), BF16)] + small
        results = [((E, D, F), BF16), ((E, D, F), BF16), ((E, F, D), BF16)] + small
        n_units = 2 * N_CHUNK
        held = pl.pallas_call(
            functools.partial(moe_kernel, dims),
            out_shape=[vm(*r) for r in held_shapes],
            in_specs=[aspec] * 8,
            out_specs=[vspec] * len(held_shapes),
            scratch_shapes=[
                vm((E, F, D), BF16), vm((E, F, D), BF16), vm((E, D, F), BF16),
                vm((2, NT, D), BF16), vm((G, 2 * K, LANES), F32),
                vm((K, T), jnp.int32), vm((K, T), jnp.int32), vm((K, T), F32),
                vm((2, K, LANES), F32), vm((NT, 2 * K), F32),
                vm((E, RW, F), F32), vm((E, RW, F), F32),
                vm((E * RW, NT), BF16), vm((G, 4 * T, LANES), BF16),
                vm((G, E * C, D), BF16),
                vm((2, NT, D), F32), vm((n_units, NQ, T, CW), F32),
                vm((n_units, 2, T, CW // 2), F32), vm((n_units, 2, T, CW), F32),
                vm((NT // LANES, K, LANES), F32), vm((G - 1, K, LANES), F32),
                dma((E + 1,)), dma((5,)), dma, dma((4,)),
                dma((2,)), dma((2, 7)), dma, dma((n_units, 5)), dma((2,)),
            ],
            compiler_params=pltpu.CompilerParams(
                collective_id=0, has_side_effects=True, vmem_limit_bytes=39 * 2 ** 20),
            name="moe_exchange",
        )(x_rows, grad_out, expert_idx.T, slot_pos.T, gate_w.T, w_gate, w_up, w_down)
        g1, g3, g2, out, gx, gg = pl.pallas_call(
            functools.partial(write_kernel, E),
            out_shape=[jax.ShapeDtypeStruct(*r) for r in results],
            in_specs=[vspec] * len(held_shapes),
            out_specs=[aspec] * len(results),
            scratch_shapes=[vm((E - EARLY, D, F), BF16), vm((E - EARLY, D, F), BF16), vm((E, F, D), BF16),
                            dma((len(results),))],
            compiler_params=pltpu.CompilerParams(vmem_limit_bytes=16 * 2 ** 20),
            name="write_results",
        )(*held)
        return out, gx, g1, g3, g2, gg.T

    return jax.shard_map(per_device, mesh=mesh,
                         in_specs=(row_spec, row_spec, row_spec, row_spec, expert_spec, expert_spec, expert_spec, row_spec),
                         out_specs=(row_spec, row_spec, row_spec, row_spec, row_spec, row_spec),
                         check_vma=False)
```

```python
import functools

import jax
import jax.numpy as jnp
from jax import lax
from jax.experimental import pallas as pl
from jax.experimental.pallas import tpu as pltpu
from jax.sharding import PartitionSpec as P

BF16, F32 = jnp.bfloat16, jnp.float32
MESH_ID = pl.DeviceIdType.MESH
LANES = 128
N_CHUNK = 3
TB = 256
EARLY = 2
SLOTS = 3


def capacity_of(tok_dev, top_k, n_experts):
    return ((2 * tok_dev * top_k + n_experts - 1) // n_experts + 7) // 8 * 8


def dot_nn(a, b):
    return lax.dot_general(a, b, (((1,), (0,)), ((), ())), preferred_element_type=F32)


def dot_nt(a, b):
    return lax.dot_general(a, b, (((1,), (1,)), ((), ())), preferred_element_type=F32)


def dot_tn(a, b):
    return lax.dot_general(a, b, (((0,), (0,)), ((), ())), preferred_element_type=F32)


def up_grads(r, dab, e, g1, g3, n):
    D, F = r.shape[2], dab.shape[2] // 2
    for m in range(0, D, TB):
        sl = pl.ds(m, TB)
        res = dot_tn(r[e, :, sl], dab[e])
        g1[n, sl, :] = res[:, 0:F].astype(BF16)
        g3[n, sl, :] = res[:, F:2 * F].astype(BF16)


def moe_kernel(dims, x_hbm, g_hbm, idx_hbm, slot_hbm, gate_hbm, w1_hbm, w3_hbm, w2_hbm,
               w1, w3, r_all, dy_all, h_all, dab_all, out_ref, gg_ref, own_ref, tor_ref, tol_ref,
               w2, w1t, w2t, xg, meta, idx_v, slot_v, gate_v, scr, tok, c1_all, c2_all,
               p_all, comb, y_all, part, sibbuf, ringbuf, finbuf, ggsrc, ggbuf,
               w_sem, loc_sem, meta_ss, meta_rs, ag_ss, ag_rs, rt_ss, rt_rs, gg_sem):
    G, T, D, F, E, C, K = dims
    NQ = G // 2
    RW, NT = G * C, G * T
    CW = D // N_CHUNK
    assert CW == F and G == 8
    per_tile = LANES // T
    me = lax.axis_index("ep")
    core = lax.rem(me, 2)
    chip = me // 2
    right_chip, left_chip, opp_chip = (lax.rem(chip + 1, NQ), lax.rem(chip + NQ - 1, NQ), lax.rem(chip + 2, NQ))
    dev = lambda q, c: q * 2 + c
    other = 1 - core
    sib = dev(chip, other)
    right, left, opp = dev(right_chip, core), dev(left_chip, core), dev(opp_chip, core)

    def rows(d):
        return pl.ds(pl.multiple_of(d * T, T), T)

    def remote(src, dst, ss, rs, target):
        return pltpu.make_async_remote_copy(src_ref=src, dst_ref=dst, send_sem=ss, recv_sem=rs,
                                            device_id={"ep": target}, device_id_type=MESH_ID)

    local = [pltpu.make_async_copy(src, dst, loc_sem.at[i]) for i, (src, dst) in enumerate((
        (idx_hbm, idx_v), (slot_hbm, slot_v), (gate_hbm, gate_v),
        (x_hbm, xg.at[0, rows(me)]), (g_hbm, xg.at[1, rows(me)])))]

    def wait_bytes(ref, sem):
        pltpu.make_async_copy(ref, ref, sem).wait()

    barrier = pltpu.get_barrier_semaphore()
    for d in (sib, right, left):
        pl.semaphore_signal(barrier, inc=1, device_id={"ep": d}, device_id_type=MESH_ID)
    scr[...] = jnp.zeros_like(scr)
    for cp in local:
        cp.start()
    for cp in local[:3]:
        cp.wait()
    off = lax.rem(me, per_tile) * T
    scr[0, :, 0:T] = jnp.where(slot_v[...] >= 0, idx_v[...] * C + slot_v[...] + 1, 0).astype(F32)
    scr[1, :, 0:T] = gate_v[...]
    meta[me, 0:K] = pltpu.roll(scr[0], off, 1)
    meta[me, K:2 * K] = pltpu.roll(scr[1], off, 1)
    local[3].wait()
    local[4].wait()
    for e in range(E):
        pltpu.make_async_copy(w1_hbm.at[e], w1.at[e], w_sem.at[e]).start()
        pltpu.make_async_copy(w2_hbm.at[e], w2.at[e], w_sem.at[e]).start()
    for e in range(E):
        pltpu.make_async_copy(w3_hbm.at[e], w3.at[e], w_sem.at[E]).start()
    pl.semaphore_wait(barrier, 3)

    lo, hi, full = pl.ds(0, D // 2), pl.ds(D // 2, D // 2), pl.ds(0, D)
    sib_right, sib_left, sib_opp = dev(right_chip, other), dev(left_chip, other), dev(opp_chip, other)
    ag_out = ((me, full, sib), (me, lo, right), (me, hi, right), (me, hi, left), (me, lo, left),
              (left, lo, right), (right, hi, left), (left, full, sib), (right, full, sib),
              (opp, lo, sib), (opp, hi, sib))
    ag_in = ((sib, full, sib), (left, lo, left), (left, hi, left), (right, hi, right), (right, lo, right),
             (opp, lo, left), (opp, hi, right), (sib_left, full, sib), (sib_right, full, sib),
             (sib_opp, lo, sib), (sib_opp, hi, sib))
    meta_out = ((me, sib), (me, right), (me, left), (left, right), (left, sib), (right, sib), (opp, sib))
    meta_in = ((sib, sib), (left, left), (right, right), (opp, left), (sib_left, sib), (sib_right, sib), (sib_opp, sib))

    def ag(table, t, k):
        src_dev, cols, target = table[k]
        ref = xg.at[t, rows(src_dev), cols]
        return remote(ref, ref, ag_ss.at[t], ag_rs.at[t, k if k < 7 else 0], target)

    def mt(table, k):
        src_dev, target = table[k]
        return remote(meta.at[src_dev], meta.at[src_dev], meta_ss, meta_rs.at[k if k < 4 else 0], target)

    def ag_send(t, *ks):
        for k in ks:
            ag(ag_out, t, k).start()

    def ag_recv(t, *ks):
        for k in ks:
            ag(ag_in, t, k).wait_recv()

    def ag_recv_sib(t):
        wait_bytes(xg.at[t, pl.ds(0, NQ * T)], ag_rs.at[t, 0])

    def mt_send(*ks):
        for k in ks:
            mt(meta_out, k).start()

    def mt_recv(*ks):
        for k in ks:
            mt(meta_in, k).wait_recv()

    ag_send(0, 1, 3)
    mt_send(1, 2, 0)
    ag_send(0, 2, 4, 0)

    def flip(dst, src):
        for i in range(0, src.shape[0], TB):
            for j in range(0, src.shape[1], TB):
                dst[pl.ds(j, TB), pl.ds(i, TB)] = src[pl.ds(i, TB), pl.ds(j, TB)].T

    def flip_12(e):
        wait_bytes(w1.at[pl.ds(0, 2)], w_sem.at[e])
        flip(w1t.at[e], w1.at[e])
        flip(w2t.at[e], w2.at[e])

    def flip_3(e):
        for b in range(0, D, F):
            for i in range(0, F, TB):
                for j in range(i, F, TB):
                    up_ref = w3.at[e, pl.ds(b + i, TB), pl.ds(j, TB)]
                    low_ref = w3.at[e, pl.ds(b + j, TB), pl.ds(i, TB)]
                    up_t, low_t = up_ref[...].T, low_ref[...].T
                    up_ref[...] = low_t
                    if i != j:
                        low_ref[...] = up_t

    flip_12(0)
    ag_recv(0, 1)
    ag_send(0, 5)
    ag_recv(0, 3)
    ag_send(0, 6)
    mt_recv(1)
    mt_send(3, 4)
    mt_recv(2)
    mt_send(5)
    ag_send(1, 1, 3, 2, 4, 0)
    flip_12(1)
    flip_12(2)
    ag_recv(0, 2)
    ag_send(0, 7)
    ag_recv(0, 4)
    ag_send(0, 8)
    mt_recv(3)
    mt_send(6)
    flip_12(3)
    ag_recv(0, 5)
    ag_send(0, 9)
    ag_recv(0, 6)
    ag_send(0, 10)
    flip_12(E - 1)
    wait_bytes(meta.at[pl.ds(0, NQ)], meta_rs.at[0])

    n_tiles = G // per_tile
    halves = []
    for i in range(n_tiles):
        tot = meta[i * per_tile]
        for s in range(i * per_tile + 1, (i + 1) * per_tile):
            tot = tot + meta[s]
        halves.append(tot)
    codes = jnp.concatenate([v[0:K] for v in halves], axis=1)
    gates = jnp.concatenate([v[K:2 * K] for v in halves], axis=1)
    lane_src = (lax.broadcasted_iota(jnp.int32, (K, NT), 1) // T * C).astype(F32)
    row_id = lax.broadcasted_iota(jnp.int32, (RW, NT), 0).astype(F32) + 1.0

    def routing(e):
        first = ((me * E + e) * C).astype(F32) + 1.0
        sel = (codes >= first) & (codes < first + float(C))
        pos = jnp.sum(jnp.where(sel, codes - first + lane_src + 1.0, 0.0), axis=0, keepdims=True)
        gate_row = jnp.sum(jnp.where(sel, gates, 0.0), axis=0, keepdims=True)
        return sel, row_id == pos, gate_row

    def erow(e):
        return pl.ds(e * RW, RW)

    for e in range(E):
        p_all[erow(e), :] = jnp.where(routing(e)[1], 1.0, 0.0).astype(BF16)

    EC = E * C

    def build_comb():
        tok[...] = jnp.transpose(jnp.concatenate([codes, gates], axis=0))
        pair = lax.broadcasted_iota(jnp.int32, (NT, LANES), 1)
        want = jnp.where(pair < EC, pair + me * EC + 1, -1).astype(F32)
        one, rest = jnp.zeros((NT, LANES), F32), jnp.zeros((NT, LANES), F32)
        for k in range(K):
            hit = tok[:, k:k + 1] == want
            one = jnp.where(hit, 1.0, one)
            rest = jnp.where(hit, tok[:, K + k:K + k + 1], rest)
        for i in range(3):
            piece = rest.astype(BF16)
            for s in range(G):
                comb[s, pl.ds(i * T, T), :] = piece[s * T:(s + 1) * T]
            rest = rest - piece.astype(F32)
        for s in range(G):
            comb[s, pl.ds(3 * T, T), :] = one[s * T:(s + 1) * T].astype(BF16)

    ag_recv_sib(0)
    wait_bytes(w3, w_sem.at[E])

    ag_recv(1, 1)
    ag_send(1, 5)
    ag_recv(1, 3)
    ag_send(1, 6)

    def select_x(e):
        r_all[e] = dot_nn(p_all[erow(e), :], xg[0]).astype(BF16)

    def up(e):
        a = dot_nn(r_all[e], w1[e])
        b = dot_nn(r_all[e], w3[e])
        s = jax.nn.sigmoid(a)
        act = a * s
        h_all[e] = (act * b).astype(BF16)
        c1_all[e] = b * (s * (1.0 + a * (1.0 - s)))
        c2_all[e] = act

    select_x(0)
    for e in range(E):
        if e + 1 < E:
            select_x(e + 1)
        up(e)
        flip_3(e)
        if e == 0:
            build_comb()
        if e == 2:
            ag_recv(1, 2)
            ag_send(1, 7)
            ag_recv(1, 4)
            ag_send(1, 8)

    chips = (opp_chip, right_chip, left_chip, chip)
    HW = CW // 2

    def cols(j):
        return pl.ds(j * CW, CW)

    def half(j, i):
        return pl.ds(j * CW + i * HW, HW)

    c_half = (pl.ds(0, HW), pl.ds(HW, HW))

    def ret_desc(t, j, n):
        u = t * N_CHUNK + j
        if n < 4:
            src, dst, tgt = part.at[t, rows(dev(chips[n], other)), cols(j)], sibbuf.at[u, n], sib
        elif n == 4:
            src, dst, tgt = part.at[t, rows(opp), half(j, 0)], ringbuf.at[u, 0], right
        elif n == 5:
            src, dst, tgt = part.at[t, rows(opp), half(j, 1)], ringbuf.at[u, 1], left
        elif n in (6, 8):
            i = 1 if n == 6 else 0
            src, dst, tgt = part.at[t, rows(right), half(j, i)], finbuf.at[u, 0, :, c_half[i]], right
        else:
            i = 0 if n == 7 else 1
            src, dst, tgt = part.at[t, rows(left), half(j, i)], finbuf.at[u, 1, :, c_half[i]], left
        return remote(src, dst, rt_ss.at[t], rt_rs.at[u, (0, 0, 0, 0, 1, 2, 3, 4, 3, 4)[n]], tgt)

    def ret_0(t, j):
        for n in range(4):
            ret_desc(t, j, n).start()

    def ret_1(t, j):
        u = t * N_CHUNK + j
        wait_bytes(sibbuf.at[u], rt_rs.at[u, 0])
        for n, d in enumerate((opp, right, left, me)):
            part[t, rows(d), cols(j)] += sibbuf[u, n]
            for m in ((4, 5), (6,), (7,), ())[n]:
                if t == 0 or m < 6:
                    ret_desc(t, j, m).start()

    def ret_2(t, j):
        u = t * N_CHUNK + j
        for n, d, i in ((4, right, 0), (5, left, 1)):
            ret_desc(t, j, n).wait_recv()
            if t == 0:
                part[t, rows(d), half(j, i)] += ringbuf[u, i]
                ret_desc(t, j, n + 4).start()
            else:
                to_ref = (tor_ref, tol_ref)[i]
                to_ref[:, half(j, i)] = part[t, rows(d), half(j, i)] + ringbuf[u, i]
                to_ref[:, half(j, 1 - i)] = part[t, rows(d), half(j, 1 - i)]
        if t == 1:
            own_ref[:, cols(j)] = part[t, rows(me), cols(j)]

    def ret_3(t, j, res_ref):
        u = t * N_CHUNK + j
        wait_bytes(finbuf.at[u, 0], rt_rs.at[u, 3])
        wait_bytes(finbuf.at[u, 1], rt_rs.at[u, 4])
        res_ref[:, cols(j)] = (part[t, rows(me), cols(j)] + finbuf[u, 0] + finbuf[u, 1]).astype(BF16)

    def put_rows(e, j, val):
        for s in range(G):
            y_all[s, pl.ds(e * C, C), cols(j)] = val[s * C:(s + 1) * C]

    def y_cols(j):
        for e in range(E):
            put_rows(e, j, dot_nn(h_all[e], w2[e, :, cols(j)]).astype(BF16))

    def combine_y(j):
        for s in range(G):
            acc = dot_nn(comb[s, 0:3 * T, 0:EC], y_all[s, :, cols(j)])
            part[0, pl.ds(s * T, T), cols(j)] = acc[0:T] + acc[T:2 * T] + acc[2 * T:3 * T]
        ret_0(0, j)

    y_cols(0)
    for j in range(N_CHUNK):
        if j + 1 < N_CHUNK:
            y_cols(j + 1)
        combine_y(j)
        if j == 0:
            ag_recv(1, 5)
            ag_send(1, 9)
            ag_recv(1, 6)
            ag_send(1, 10)

    ag_recv_sib(1)

    gg = jnp.zeros((K, NT), F32)

    def select_g(e, gg):
        sel, mask, gate_row = routing(e)
        gate_col = jnp.sum(jnp.where(mask, gate_row, 0.0), axis=1, keepdims=True)
        g_e = dot_nn(p_all[erow(e), :], xg[1])
        dy_all[e] = (gate_col * g_e).astype(BF16)
        y_e = y_all[:, pl.ds(e * C, C), :].reshape(RW, D)
        gg_col = jnp.sum(g_e * y_e.astype(F32), axis=1, keepdims=True)
        gg_row = jnp.sum(jnp.where(mask, gg_col, 0.0), axis=0, keepdims=True)
        return gg + jnp.where(sel, gg_row, 0.0)

    def down_t(e):
        dh = dot_nn(dy_all[e], w2t[e])
        dab_all[e, :, 0:F] = (dh * c1_all[e]).astype(BF16)
        dab_all[e, :, F:2 * F] = (dh * c2_all[e]).astype(BF16)

    ret_1(0, 0)
    gg = select_g(0, gg)
    for e in range(E):
        if e + 1 < E:
            gg = select_g(e + 1, gg)
        down_t(e)
        if e + 1 < N_CHUNK:
            ret_1(0, e + 1)
    for i in range(n_tiles):
        ggsrc[i] = gg[:, i * LANES:(i + 1) * LANES]

    def gg_desc(d):
        tgt = lax.rem(me + d, G)
        return remote(ggsrc.at[tgt // per_tile], ggbuf.at[d - 1], gg_sem.at[0], gg_sem.at[1], tgt)

    for d in range(1, G):
        gg_desc(d).start()

    def dr_cols(j):
        for e in range(E):
            dr = dot_nn(dab_all[e, :, 0:F], w1t[e, :, cols(j)]) + dot_nn(dab_all[e, :, F:2 * F], w3[e, cols(j), :])
            put_rows(e, j, dr.astype(BF16))

    def combine_dr(j):
        for s in range(G):
            part[1, pl.ds(s * T, T), cols(j)] = dot_nn(comb[s, 3 * T:4 * T, 0:EC], y_all[s, :, cols(j)])
        ret_0(1, j)

    dr_cols(0)
    for j in range(N_CHUNK):
        if j + 1 < N_CHUNK:
            dr_cols(j + 1)
        combine_dr(j)
        if j + 1 == N_CHUNK:
            ret_1(1, 0)
        ret_2(0, j)

    ret_1(1, 1)
    ret_1(1, 2)
    up_grads(r_all, dab_all, 0, w1, w3, 0)
    up_grads(r_all, dab_all, 1, w1, w3, 1)
    ret_2(1, 0)
    for j in range(N_CHUNK):
        ret_3(0, j, out_ref)
    ret_2(1, 1)
    for e in range(2, EARLY):
        up_grads(r_all, dab_all, e, w1, w3, e)
    tot = ggsrc[me // per_tile]
    wait_bytes(ggbuf, gg_sem.at[1])
    for d in range(1, G):
        tot = tot + ggbuf[d - 1]
    gg_ref[...] = pltpu.roll(tot, lax.rem(LANES - off, LANES), 1)[:, 0:T]
    ret_2(1, 2)
    sent = pl.ds(0, (G - 1) * T)
    wait_bytes(meta.at[pl.ds(0, G - 1)], meta_ss)
    wait_bytes(xg.at[0, sent], ag_ss.at[0])
    wait_bytes(xg.at[1, sent], ag_ss.at[1])
    wait_bytes(ggbuf, gg_sem.at[0])
    wait_bytes(part.at[0, sent], rt_ss.at[0])
    wait_bytes(part.at[1, pl.ds(0, (NQ + 1) * T)], rt_ss.at[1])


def write_kernel(n_exp, g1, g3, r, dy, h, dab, out, gg, g1_hbm, g3_hbm, g2_hbm, out_hbm, gg_hbm,
                 late1, late3, g2, sem):
    def send(src, dst, k):
        pltpu.make_async_copy(src, dst, sem.at[k]).start()

    for e in range(EARLY):
        send(g1.at[e], g1_hbm.at[e], 0)
        send(g3.at[e], g3_hbm.at[e], 1)
    send(out, out_hbm, 2)
    send(gg, gg_hbm, 3)
    F = h.shape[2]

    def down_copy(e):
        return pltpu.make_async_copy(g2.at[e % SLOTS], g2_hbm.at[e], sem.at[4 + e % SLOTS])

    for e in range(n_exp):
        if e >= SLOTS:
            down_copy(e - SLOTS).wait()
        for m in range(0, F, TB):
            g2[e % SLOTS, pl.ds(m, TB), :] = dot_tn(h[e, :, pl.ds(m, TB)], dy[e]).astype(BF16)
        down_copy(e).start()
        if e >= EARLY:
            n = e - EARLY
            up_grads(r, dab, e, late1, late3, n)
            send(late1.at[n], g1_hbm.at[e], 0)
            send(late3.at[n], g3_hbm.at[e], 1)
    for e in range(n_exp - SLOTS, n_exp):
        down_copy(e).wait()
    for k, ref in enumerate((g1_hbm, g3_hbm, out_hbm, gg_hbm)):
        pltpu.make_async_copy(ref, ref, sem.at[k]).wait()


def add_kernel(own, from_left, from_right, gx):
    gx[...] = (own[...] + from_left[...] + from_right[...]).astype(BF16)


def solution(mesh):
    group_size = mesh.shape['ep']
    row_spec = P(('dp', 'ep'))
    expert_spec = P('ep')

    def per_device(x_rows, expert_idx, gate_w, slot_pos, w_gate, w_up, w_down, grad_out):
        T, D = x_rows.shape
        K = expert_idx.shape[1]
        E, _, F = w_gate.shape
        G = group_size
        C = capacity_of(T, K, E * G)
        RW, NT = G * C, G * T
        NQ = G // 2
        CW = D // N_CHUNK
        dims = (G, T, D, F, E, C, K)
        vm = pltpu.VMEM
        dma = pltpu.SemaphoreType.DMA
        vspec = pl.BlockSpec(memory_space=pltpu.VMEM)
        aspec = pl.BlockSpec(memory_space=pl.ANY)
        small = [((T, D), BF16), ((K, T), F32)]
        partial = [((T, D), F32)] * 3
        held_shapes = [((E, D, F), BF16), ((E, D, F), BF16), ((E, RW, D), BF16), ((E, RW, D), BF16),
                       ((E, RW, F), BF16), ((E, RW, 2 * F), BF16)] + small + partial
        results = [((E, D, F), BF16), ((E, D, F), BF16), ((E, F, D), BF16)] + small
        n_units = 2 * N_CHUNK
        *held, own, to_right, to_left = pl.pallas_call(
            functools.partial(moe_kernel, dims),
            out_shape=[vm(*r) for r in held_shapes],
            in_specs=[aspec] * 8,
            out_specs=[vspec] * len(held_shapes),
            scratch_shapes=[
                vm((E, F, D), BF16), vm((E, F, D), BF16), vm((E, D, F), BF16),
                vm((2, NT, D), BF16), vm((G, 2 * K, LANES), F32),
                vm((K, T), jnp.int32), vm((K, T), jnp.int32), vm((K, T), F32),
                vm((2, K, LANES), F32), vm((NT, 2 * K), F32),
                vm((E, RW, F), F32), vm((E, RW, F), F32),
                vm((E * RW, NT), BF16), vm((G, 4 * T, LANES), BF16),
                vm((G, E * C, D), BF16),
                vm((2, NT, D), F32), vm((n_units, NQ, T, CW), F32),
                vm((n_units, 2, T, CW // 2), F32), vm((N_CHUNK, 2, T, CW), F32),
                vm((NT // LANES, K, LANES), F32), vm((G - 1, K, LANES), F32),
                dma((E + 1,)), dma((5,)), dma, dma((4,)),
                dma((2,)), dma((2, 7)), dma((2,)), dma((n_units, 5)), dma((2,)),
            ],
            compiler_params=pltpu.CompilerParams(
                collective_id=0, has_side_effects=True, vmem_limit_bytes=39 * 2 ** 20),
            name="moe_exchange",
        )(x_rows, grad_out, expert_idx.T, slot_pos.T, gate_w.T, w_gate, w_up, w_down)
        ahead = [(d, (d + 2) % G) for d in range(G)]
        from_left = lax.ppermute(to_right, 'ep', ahead)
        from_right = lax.ppermute(to_left, 'ep', [(b, a) for a, b in ahead])
        g1, g3, g2, out, gg = pl.pallas_call(
            functools.partial(write_kernel, E),
            out_shape=[jax.ShapeDtypeStruct(*r) for r in results],
            in_specs=[vspec] * len(held),
            out_specs=[aspec] * len(results),
            scratch_shapes=[vm((E - EARLY, D, F), BF16), vm((E - EARLY, D, F), BF16), vm((SLOTS, F, D), BF16),
                            dma((4 + SLOTS,))],
            compiler_params=pltpu.CompilerParams(vmem_limit_bytes=15 * 2 ** 20),
            cost_estimate=pl.CostEstimate(flops=4 * E * RW * D * F, bytes_accessed=6 * E * D * F, transcendentals=0),
            name="write_results",
        )(*held)
        gx = pl.pallas_call(
            add_kernel,
            out_shape=jax.ShapeDtypeStruct((T, D), BF16),
            in_specs=[vspec] * 3,
            out_specs=vspec,
            compiler_params=pltpu.CompilerParams(vmem_limit_bytes=2 ** 21),
            name="add_partials",
        )(own, from_left, from_right)
        return out, gx, g1, g3, g2, gg.T

    return jax.shard_map(per_device, mesh=mesh,
                         in_specs=(row_spec, row_spec, row_spec, row_spec, expert_spec, expert_spec, expert_spec, row_spec),
                         out_specs=(row_spec, row_spec, row_spec, row_spec, row_spec, row_spec),
                         check_vma=False)
```

```python
import functools

import jax
import jax.numpy as jnp
from jax import lax
from jax.experimental import pallas as pl
from jax.experimental.pallas import tpu as pltpu
from jax.sharding import PartitionSpec as P

BF16, F32 = jnp.bfloat16, jnp.float32
MESH_ID = pl.DeviceIdType.MESH
LANES = 128
N_CHUNK = 3
TB = 256
EARLY = 3


def capacity_of(tok_dev, top_k, n_experts):
    return ((2 * tok_dev * top_k + n_experts - 1) // n_experts + 7) // 8 * 8


def dot_nn(a, b):
    return lax.dot_general(a, b, (((1,), (0,)), ((), ())), preferred_element_type=F32)


def dot_nt(a, b):
    return lax.dot_general(a, b, (((1,), (1,)), ((), ())), preferred_element_type=F32)


def dot_tn(a, b):
    return lax.dot_general(a, b, (((0,), (0,)), ((), ())), preferred_element_type=F32)


def up_grads(r, dab, e, g1, g3, n):
    D, F = r.shape[2], dab.shape[2] // 2
    for m in range(0, D, TB):
        sl = pl.ds(m, TB)
        res = dot_tn(r[e, :, sl], dab[e])
        g1[n, sl, :] = res[:, 0:F].astype(BF16)
        g3[n, sl, :] = res[:, F:2 * F].astype(BF16)


def moe_kernel(dims, x_hbm, g_hbm, idx_hbm, slot_hbm, gate_hbm, w1_hbm, w3_hbm, w2_hbm,
               w1, w3, r_all, dy_all, h_all, dab_all, out_ref, gg_ref, own_ref, tor_ref, tol_ref,
               w2, w1t, w2t, xg, meta, idx_v, slot_v, gate_v, scr, tok, c1_all, c2_all,
               p_all, comb, y_all, part, sibbuf, ringbuf, finbuf, ggsrc, ggbuf,
               w_sem, loc_sem, meta_ss, meta_rs, ag_ss, ag_rs, rt_ss, rt_rs, fin_sem, gg_sem):
    G, T, D, F, E, C, K = dims
    NQ = G // 2
    RW, NT = G * C, G * T
    CW = D // N_CHUNK
    assert CW == F and G == 8
    per_tile = LANES // T
    me = lax.axis_index("ep")
    core = lax.rem(me, 2)
    chip = me // 2
    right_chip, left_chip, opp_chip = (lax.rem(chip + 1, NQ), lax.rem(chip + NQ - 1, NQ), lax.rem(chip + 2, NQ))
    dev = lambda q, c: q * 2 + c
    other = 1 - core
    sib = dev(chip, other)
    right, left, opp = dev(right_chip, core), dev(left_chip, core), dev(opp_chip, core)

    def rows(d):
        return pl.ds(pl.multiple_of(d * T, T), T)

    def remote(src, dst, ss, rs, target):
        return pltpu.make_async_remote_copy(src_ref=src, dst_ref=dst, send_sem=ss, recv_sem=rs,
                                            device_id={"ep": target}, device_id_type=MESH_ID)

    local = [pltpu.make_async_copy(src, dst, loc_sem.at[i]) for i, (src, dst) in enumerate((
        (idx_hbm, idx_v), (slot_hbm, slot_v), (gate_hbm, gate_v),
        (x_hbm, xg.at[0, rows(me)]), (g_hbm, xg.at[1, rows(me)])))]

    def wait_bytes(ref, sem):
        pltpu.make_async_copy(ref, ref, sem).wait()

    barrier = pltpu.get_barrier_semaphore()
    for d in (sib, right, left):
        pl.semaphore_signal(barrier, inc=1, device_id={"ep": d}, device_id_type=MESH_ID)
    scr[...] = jnp.zeros_like(scr)
    for cp in local:
        cp.start()
    for cp in local[:3]:
        cp.wait()
    off = lax.rem(me, per_tile) * T
    scr[0, :, 0:T] = jnp.where(slot_v[...] >= 0, idx_v[...] * C + slot_v[...] + 1, 0).astype(F32)
    scr[1, :, 0:T] = gate_v[...]
    meta[me, 0:K] = pltpu.roll(scr[0], off, 1)
    meta[me, K:2 * K] = pltpu.roll(scr[1], off, 1)
    local[3].wait()
    local[4].wait()
    for e in range(E):
        pltpu.make_async_copy(w1_hbm.at[e], w1.at[e], w_sem.at[e]).start()
        pltpu.make_async_copy(w2_hbm.at[e], w2.at[e], w_sem.at[e]).start()
    for e in range(E):
        pltpu.make_async_copy(w3_hbm.at[e], w3.at[e], w_sem.at[E]).start()
    pl.semaphore_wait(barrier, 3)

    lo, hi, full = pl.ds(0, D // 2), pl.ds(D // 2, D // 2), pl.ds(0, D)
    sib_right, sib_left, sib_opp = dev(right_chip, other), dev(left_chip, other), dev(opp_chip, other)
    ag_out = ((me, full, sib), (me, lo, right), (me, hi, right), (me, hi, left), (me, lo, left),
              (left, lo, right), (right, hi, left), (left, full, sib), (right, full, sib),
              (opp, lo, sib), (opp, hi, sib))
    ag_in = ((sib, full, sib), (left, lo, left), (left, hi, left), (right, hi, right), (right, lo, right),
             (opp, lo, left), (opp, hi, right), (sib_left, full, sib), (sib_right, full, sib),
             (sib_opp, lo, sib), (sib_opp, hi, sib))
    meta_out = ((me, sib), (me, right), (me, left), (left, right), (left, sib), (right, sib), (opp, sib))
    meta_in = ((sib, sib), (left, left), (right, right), (opp, left), (sib_left, sib), (sib_right, sib), (sib_opp, sib))

    def ag(table, t, k):
        src_dev, cols, target = table[k]
        ref = xg.at[t, rows(src_dev), cols]
        return remote(ref, ref, ag_ss.at[t], ag_rs.at[t, k if k < 7 else 0], target)

    def mt(table, k):
        src_dev, target = table[k]
        return remote(meta.at[src_dev], meta.at[src_dev], meta_ss, meta_rs.at[k if k < 4 else 0], target)

    def ag_send(t, *ks):
        for k in ks:
            ag(ag_out, t, k).start()

    def ag_recv(t, *ks):
        for k in ks:
            ag(ag_in, t, k).wait_recv()

    def ag_recv_sib(t):
        wait_bytes(xg.at[t, pl.ds(0, NQ * T)], ag_rs.at[t, 0])

    def mt_send(*ks):
        for k in ks:
            mt(meta_out, k).start()

    def mt_recv(*ks):
        for k in ks:
            mt(meta_in, k).wait_recv()

    ag_send(0, 1, 3)
    mt_send(1, 2, 0)
    ag_send(0, 2, 4, 0)

    def flip(dst, src):
        for i in range(0, src.shape[0], TB):
            for j in range(0, src.shape[1], TB):
                dst[pl.ds(j, TB), pl.ds(i, TB)] = src[pl.ds(i, TB), pl.ds(j, TB)].T

    def flip_12(e):
        wait_bytes(w1.at[pl.ds(0, 2)], w_sem.at[e])
        flip(w1t.at[e], w1.at[e])
        flip(w2t.at[e], w2.at[e])

    def flip_3(e):
        for b in range(0, D, F):
            for i in range(0, F, TB):
                for j in range(i, F, TB):
                    up_ref = w3.at[e, pl.ds(b + i, TB), pl.ds(j, TB)]
                    low_ref = w3.at[e, pl.ds(b + j, TB), pl.ds(i, TB)]
                    up_t, low_t = up_ref[...].T, low_ref[...].T
                    up_ref[...] = low_t
                    if i != j:
                        low_ref[...] = up_t

    flip_12(0)
    ag_recv(0, 1)
    ag_send(0, 5)
    ag_recv(0, 3)
    ag_send(0, 6)
    mt_recv(1)
    mt_send(3, 4)
    mt_recv(2)
    mt_send(5)
    ag_send(1, 1, 3, 2, 4, 0)
    flip_12(1)
    flip_12(2)
    ag_recv(0, 2)
    ag_send(0, 7)
    ag_recv(0, 4)
    ag_send(0, 8)
    mt_recv(3)
    mt_send(6)
    flip_12(3)
    ag_recv(0, 5)
    ag_send(0, 9)
    ag_recv(0, 6)
    ag_send(0, 10)
    flip_12(E - 1)
    wait_bytes(meta.at[pl.ds(0, NQ)], meta_rs.at[0])

    n_tiles = G // per_tile
    halves = []
    for i in range(n_tiles):
        tot = meta[i * per_tile]
        for s in range(i * per_tile + 1, (i + 1) * per_tile):
            tot = tot + meta[s]
        halves.append(tot)
    codes = jnp.concatenate([v[0:K] for v in halves], axis=1)
    gates = jnp.concatenate([v[K:2 * K] for v in halves], axis=1)
    lane_src = (lax.broadcasted_iota(jnp.int32, (K, NT), 1) // T * C).astype(F32)
    row_id = lax.broadcasted_iota(jnp.int32, (RW, NT), 0).astype(F32) + 1.0

    def routing(e):
        first = ((me * E + e) * C).astype(F32) + 1.0
        sel = (codes >= first) & (codes < first + float(C))
        pos = jnp.sum(jnp.where(sel, codes - first + lane_src + 1.0, 0.0), axis=0, keepdims=True)
        gate_row = jnp.sum(jnp.where(sel, gates, 0.0), axis=0, keepdims=True)
        return sel, row_id == pos, gate_row

    def erow(e):
        return pl.ds(e * RW, RW)

    for e in range(E):
        p_all[erow(e), :] = jnp.where(routing(e)[1], 1.0, 0.0).astype(BF16)

    EC = E * C

    def build_comb():
        tok[...] = jnp.transpose(jnp.concatenate([codes, gates], axis=0))
        pair = lax.broadcasted_iota(jnp.int32, (NT, LANES), 1)
        want = jnp.where(pair < EC, pair + me * EC + 1, -1).astype(F32)
        one, rest = jnp.zeros((NT, LANES), F32), jnp.zeros((NT, LANES), F32)
        for k in range(K):
            hit = tok[:, k:k + 1] == want
            one = jnp.where(hit, 1.0, one)
            rest = jnp.where(hit, tok[:, K + k:K + k + 1], rest)
        for i in range(3):
            piece = rest.astype(BF16)
            for s in range(G):
                comb[s, pl.ds(i * T, T), :] = piece[s * T:(s + 1) * T]
            rest = rest - piece.astype(F32)
        for s in range(G):
            comb[s, pl.ds(3 * T, T), :] = one[s * T:(s + 1) * T].astype(BF16)

    ag_recv_sib(0)
    wait_bytes(w3, w_sem.at[E])

    ag_recv(1, 1)
    ag_send(1, 5)
    ag_recv(1, 3)
    ag_send(1, 6)

    def select_x(e):
        r_all[e] = dot_nn(p_all[erow(e), :], xg[0]).astype(BF16)

    def up(e):
        a = dot_nn(r_all[e], w1[e])
        b = dot_nn(r_all[e], w3[e])
        s = jax.nn.sigmoid(a)
        act = a * s
        h_all[e] = (act * b).astype(BF16)
        c1_all[e] = b * (s * (1.0 + a * (1.0 - s)))
        c2_all[e] = act

    select_x(0)
    for e in range(E):
        if e + 1 < E:
            select_x(e + 1)
        up(e)
        flip_3(e)
        if e == 0:
            build_comb()
        if e == 2:
            ag_recv(1, 2)
            ag_send(1, 7)
            ag_recv(1, 4)
            ag_send(1, 8)

    chips = (opp_chip, right_chip, left_chip, chip)
    HW = CW // 2

    def cols(j):
        return pl.ds(j * CW, CW)

    def half(j, i):
        return pl.ds(j * CW + i * HW, HW)

    c_half = (pl.ds(0, HW), pl.ds(HW, HW))

    def ret_desc(t, j, n):
        u = t * N_CHUNK + j
        if n < 4:
            src, dst, tgt = part.at[t, rows(dev(chips[n], other)), cols(j)], sibbuf.at[u, n], sib
        elif n == 4:
            src, dst, tgt = part.at[t, rows(opp), half(j, 0)], ringbuf.at[u, 0], right
        elif n == 5:
            src, dst, tgt = part.at[t, rows(opp), half(j, 1)], ringbuf.at[u, 1], left
        elif n in (6, 8):
            i = 1 if n == 6 else 0
            src, dst, tgt = part.at[t, rows(right), half(j, i)], finbuf.at[u, 0, :, c_half[i]], right
        else:
            i = 0 if n == 7 else 1
            src, dst, tgt = part.at[t, rows(left), half(j, i)], finbuf.at[u, 1, :, c_half[i]], left
        rs = fin_sem if n > 5 else rt_rs.at[u, (3, 0, 0, 0, 1, 2)[n]]
        return remote(src, dst, rt_ss.at[t], rs, tgt)

    def ret_0(t, j):
        for n in range(4):
            ret_desc(t, j, n).start()

    def ret_1(t, j):
        u = t * N_CHUNK + j
        for n, d in enumerate((opp, right, left, me)):
            if n == 0:
                wait_bytes(sibbuf.at[u, 0], rt_rs.at[u, 3])
            if n == 1:
                wait_bytes(sibbuf.at[u, pl.ds(1, NQ - 1)], rt_rs.at[u, 0])
            part[t, rows(d), cols(j)] += sibbuf[u, n]
            for m in ((4, 5), (6,), (7,), ())[n]:
                if t == 0 or m < 6:
                    ret_desc(t, j, m).start()

    def ret_2(t, j):
        u = t * N_CHUNK + j
        for n, d, i in ((4, right, 0), (5, left, 1)):
            ret_desc(t, j, n).wait_recv()
            if t == 0:
                part[t, rows(d), half(j, i)] += ringbuf[u, i]
                ret_desc(t, j, n + 4).start()
            else:
                to_ref = (tor_ref, tol_ref)[i]
                to_ref[:, half(j, i)] = part[t, rows(d), half(j, i)] + ringbuf[u, i]
                to_ref[:, half(j, 1 - i)] = part[t, rows(d), half(j, 1 - i)]
        if t == 1:
            own_ref[:, cols(j)] = part[t, rows(me), cols(j)]

    def ret_3(t, j, res_ref):
        u = t * N_CHUNK + j
        res_ref[:, cols(j)] = (part[t, rows(me), cols(j)] + finbuf[u, 0] + finbuf[u, 1]).astype(BF16)

    def put_rows(e, j, val):
        for s in range(G):
            y_all[s, pl.ds(e * C, C), cols(j)] = val[s * C:(s + 1) * C]

    def y_cols(j):
        for e in range(E):
            put_rows(e, j, dot_nn(h_all[e], w2[e, :, cols(j)]).astype(BF16))

    def combine_y(j):
        for s in range(G):
            acc = dot_nn(comb[s, 0:3 * T, 0:EC], y_all[s, :, cols(j)])
            part[0, pl.ds(s * T, T), cols(j)] = acc[0:T] + acc[T:2 * T] + acc[2 * T:3 * T]
        ret_0(0, j)

    y_cols(0)
    for j in range(N_CHUNK):
        if j + 1 < N_CHUNK:
            y_cols(j + 1)
        combine_y(j)
        if j == 0:
            ag_recv(1, 5)
            ag_send(1, 9)
            ag_recv(1, 6)
            ag_send(1, 10)

    ag_recv_sib(1)

    gg = jnp.zeros((K, NT), F32)

    def select_g(e, gg):
        sel, mask, gate_row = routing(e)
        gate_col = jnp.sum(jnp.where(mask, gate_row, 0.0), axis=1, keepdims=True)
        g_e = dot_nn(p_all[erow(e), :], xg[1])
        dy_all[e] = (gate_col * g_e).astype(BF16)
        y_e = y_all[:, pl.ds(e * C, C), :].reshape(RW, D)
        gg_col = jnp.sum(g_e * y_e.astype(F32), axis=1, keepdims=True)
        gg_row = jnp.sum(jnp.where(mask, gg_col, 0.0), axis=0, keepdims=True)
        return gg + jnp.where(sel, gg_row, 0.0)

    def down_t(e):
        dh = dot_nn(dy_all[e], w2t[e])
        dab_all[e, :, 0:F] = (dh * c1_all[e]).astype(BF16)
        dab_all[e, :, F:2 * F] = (dh * c2_all[e]).astype(BF16)

    ret_1(0, 0)
    gg = select_g(0, gg)
    for e in range(E):
        if e + 1 < E:
            gg = select_g(e + 1, gg)
        down_t(e)
        if e + 1 < N_CHUNK:
            ret_1(0, e + 1)
    for i in range(n_tiles):
        ggsrc[i] = gg[:, i * LANES:(i + 1) * LANES]

    def gg_desc(d):
        tgt = lax.rem(me + d, G)
        return remote(ggsrc.at[tgt // per_tile], ggbuf.at[d - 1], gg_sem.at[0], gg_sem.at[1], tgt)

    for d in range(1, G):
        gg_desc(d).start()

    def dr_cols(j):
        for e in range(E):
            dr = dot_nn(dab_all[e, :, 0:F], w1t[e, :, cols(j)]) + dot_nn(dab_all[e, :, F:2 * F], w3[e, cols(j), :])
            put_rows(e, j, dr.astype(BF16))

    def combine_dr(j):
        for s in range(G):
            part[1, pl.ds(s * T, T), cols(j)] = dot_nn(comb[s, 3 * T:4 * T, 0:EC], y_all[s, :, cols(j)])
        ret_0(1, j)

    dr_cols(0)
    for j in range(N_CHUNK):
        if j + 1 < N_CHUNK:
            dr_cols(j + 1)
        combine_dr(j)
        if j + 1 == N_CHUNK:
            ret_1(1, 0)
        ret_2(0, j)

    ret_1(1, 1)
    ret_1(1, 2)
    up_grads(r_all, dab_all, 0, w1, w3, 0)
    for e in range(1, EARLY):
        up_grads(r_all, dab_all, e, w1, w3, e)
    ret_2(1, 0)
    wait_bytes(finbuf, fin_sem)
    for j in range(N_CHUNK):
        ret_3(0, j, out_ref)
    ret_2(1, 1)
    tot = ggsrc[me // per_tile]
    wait_bytes(ggbuf, gg_sem.at[1])
    for d in range(1, G):
        tot = tot + ggbuf[d - 1]
    gg_ref[...] = pltpu.roll(tot, lax.rem(LANES - off, LANES), 1)[:, 0:T]
    ret_2(1, 2)
    sent = pl.ds(0, (G - 1) * T)
    wait_bytes(meta.at[pl.ds(0, G - 1)], meta_ss)
    wait_bytes(xg.at[0, sent], ag_ss.at[0])
    wait_bytes(xg.at[1, sent], ag_ss.at[1])
    wait_bytes(ggbuf, gg_sem.at[0])
    wait_bytes(part.at[0, sent], rt_ss.at[0])
    wait_bytes(part.at[1, pl.ds(0, (NQ + 1) * T)], rt_ss.at[1])


def write_kernel(n_exp, g1, g3, r, dy, h, dab, out, gg, g1_hbm, g3_hbm, g2_hbm, out_hbm, gg_hbm,
                 late1, late3, g2, sem):
    def send(src, dst, k):
        pltpu.make_async_copy(src, dst, sem.at[k]).start()

    for e in range(EARLY):
        send(g1.at[e], g1_hbm.at[e], 0)
        send(g3.at[e], g3_hbm.at[e], 1)
    send(out, out_hbm, 3)
    send(gg, gg_hbm, 4)
    for e in range(EARLY, n_exp):
        n = e - EARLY
        up_grads(r, dab, e, late1, late3, n)
        send(late1.at[n], g1_hbm.at[e], 0)
        send(late3.at[n], g3_hbm.at[e], 1)
    F = h.shape[2]
    for e in range(n_exp):
        for m in range(0, F, TB):
            g2[e, pl.ds(m, TB), :] = dot_tn(h[e, :, pl.ds(m, TB)], dy[e]).astype(BF16)
        send(g2.at[e], g2_hbm.at[e], 2)
    for k, ref in enumerate((g1_hbm, g3_hbm, g2_hbm, out_hbm, gg_hbm)):
        pltpu.make_async_copy(ref, ref, sem.at[k]).wait()


def add_kernel(own, from_left, from_right, gx):
    gx[...] = (own[...] + from_left[...] + from_right[...]).astype(BF16)


def solution(mesh):
    group_size = mesh.shape['ep']
    row_spec = P(('dp', 'ep'))
    expert_spec = P('ep')

    def per_device(x_rows, expert_idx, gate_w, slot_pos, w_gate, w_up, w_down, grad_out):
        T, D = x_rows.shape
        K = expert_idx.shape[1]
        E, _, F = w_gate.shape
        G = group_size
        C = capacity_of(T, K, E * G)
        RW, NT = G * C, G * T
        NQ = G // 2
        CW = D // N_CHUNK
        dims = (G, T, D, F, E, C, K)
        vm = pltpu.VMEM
        dma = pltpu.SemaphoreType.DMA
        vspec = pl.BlockSpec(memory_space=pltpu.VMEM)
        aspec = pl.BlockSpec(memory_space=pl.ANY)
        small = [((T, D), BF16), ((K, T), F32)]
        partial = [((T, D), F32)] * 3
        held_shapes = [((E, D, F), BF16), ((E, D, F), BF16), ((E, RW, D), BF16), ((E, RW, D), BF16),
                       ((E, RW, F), BF16), ((E, RW, 2 * F), BF16)] + small + partial
        results = [((E, D, F), BF16), ((E, D, F), BF16), ((E, F, D), BF16)] + small
        n_units = 2 * N_CHUNK
        *held, own, to_right, to_left = pl.pallas_call(
            functools.partial(moe_kernel, dims),
            out_shape=[vm(*r) for r in held_shapes],
            in_specs=[aspec] * 8,
            out_specs=[vspec] * len(held_shapes),
            scratch_shapes=[
                vm((E, F, D), BF16), vm((E, F, D), BF16), vm((E, D, F), BF16),
                vm((2, NT, D), BF16), vm((G, 2 * K, LANES), F32),
                vm((K, T), jnp.int32), vm((K, T), jnp.int32), vm((K, T), F32),
                vm((2, K, LANES), F32), vm((NT, 2 * K), F32),
                vm((E, RW, F), F32), vm((E, RW, F), F32),
                vm((E * RW, NT), BF16), vm((G, 4 * T, LANES), BF16),
                vm((G, E * C, D), BF16),
                vm((2, NT, D), F32), vm((n_units, NQ, T, CW), F32),
                vm((n_units, 2, T, CW // 2), F32), vm((N_CHUNK, 2, T, CW), F32),
                vm((NT // LANES, K, LANES), F32), vm((G - 1, K, LANES), F32),
                dma((E + 1,)), dma((5,)), dma, dma((4,)),
                dma((2,)), dma((2, 7)), dma((2,)), dma((n_units, 4)), dma, dma((2,)),
            ],
            compiler_params=pltpu.CompilerParams(
                collective_id=0, has_side_effects=True, vmem_limit_bytes=39 * 2 ** 20),
            name="moe_exchange",
        )(x_rows, grad_out, expert_idx.T, slot_pos.T, gate_w.T, w_gate, w_up, w_down)
        ahead = [(d, (d + 2) % G) for d in range(G)]
        from_left = lax.ppermute(to_right, 'ep', ahead)
        from_right = lax.ppermute(to_left, 'ep', [(b, a) for a, b in ahead])
        g1, g3, g2, out, gg = pl.pallas_call(
            functools.partial(write_kernel, E),
            out_shape=[jax.ShapeDtypeStruct(*r) for r in results],
            in_specs=[vspec] * len(held),
            out_specs=[aspec] * len(results),
            scratch_shapes=[vm((E - EARLY, D, F), BF16), vm((E - EARLY, D, F), BF16), vm((E, F, D), BF16),
                            dma((len(results),))],
            compiler_params=pltpu.CompilerParams(vmem_limit_bytes=15 * 2 ** 20),
            cost_estimate=pl.CostEstimate(flops=4 * E * RW * D * F, bytes_accessed=6 * E * D * F, transcendentals=0),
            name="write_results",
        )(*held)
        gx = pl.pallas_call(
            add_kernel,
            out_shape=jax.ShapeDtypeStruct((T, D), BF16),
            in_specs=[vspec] * 3,
            out_specs=vspec,
            compiler_params=pltpu.CompilerParams(vmem_limit_bytes=2 ** 21),
            name="add_partials",
        )(own, from_left, from_right)
        return out, gx, g1, g3, g2, gg.T

    return jax.shard_map(per_device, mesh=mesh,
                         in_specs=(row_spec, row_spec, row_spec, row_spec, expert_spec, expert_spec, expert_spec, row_spec),
                         out_specs=(row_spec, row_spec, row_spec, row_spec, row_spec, row_spec),
                         check_vma=False)
```
